256 devices in a mesh: src: 8 (over z), tgt: 32 (over x, y, core).
Axes of the slice: x: 4, y: 4, z: 8, core: 2. Of those that a mesh axis runs over, the one named last changes fastest.
Arguments:
- generator: int32 [64], replicated, may hold values from 1 to 16383, as said below
- shift: float32 [64], replicated, may hold values from 0 to 1
- targets: float32 [64, 32768], P(None, 'tgt'), may hold values from -8 to 8
- log_weights: float32 [32768], P('tgt'), may hold values from -20 to 150
Outputs:
- potential_f: float32 [16384], P('src')
- potential_g: float32 [32768], P('tgt')
The draws below stay inside these ranges and needn't reach their ends.
Inputs may be any that keep to these rules, and one draw needn't show every extreme that they name: `generator`: odd integers.
All inputs are finite; a program needn't handle non-finite values.
Results may differ from the reference program's by a relative error of at most 0.0003.
Values sent between devices are 32-bit elements; how exact they have to be, the bound alone decides.
No kernel may reach another device: no remote copies, remote signals or barrier semaphores. Data moves between devices by JAX's collectives and lax.ppermute only.
A program may use at most 64 MiB of HBM per device.

```python
import math
import jax
import jax.numpy as jnp
from jax import lax

DIM = 64
ITERS = 2
NS = 16384
NT = 32768


def draw_generator(key, part):
    return 2 * jax.random.randint(key, (DIM,), 0, NS // 2, dtype=jnp.int32) + 1


def draw_targets(key, part):
    first = jax.random.fold_in(jax.random.fold_in(key, 11), 0)
    base = 0.6 * jax.random.normal(first, (DIM, NT), jnp.float32)
    return jnp.clip(base, -8.0, 8.0)


def draw_log_weights(key, part):
    rising = 1.1 * jnp.arange(NT, dtype=jnp.float32) / NT
    noise = 3.0 * jax.random.normal(jax.random.fold_in(key, 23), (NT,), jnp.float32)
    return jnp.clip(noise, -12.0, 12.0) + rising


def setup_inputs(seed: int = 0) -> dict:
    key_of = jax.random.split(jax.random.key(seed), 5)
    generator = draw_generator(jax.random.fold_in(key_of[4], 71), 0)
    shift = jnp.clip(jax.random.uniform(key_of[1], (DIM,), jnp.float32, 0.0, 1.0), 0.0, 1.0)
    targets = draw_targets(jax.random.fold_in(key_of[4], 71), 0)
    log_weights = draw_log_weights(jax.random.fold_in(key_of[4], 71), 0)
    return dict(generator=generator, shift=shift, targets=targets, log_weights=log_weights)


blur_level = 0.1
highest = lax.Precision.HIGHEST


def lattice_block(generator, shift, start, count, modulus):
    index = start + jnp.arange(count, dtype=jnp.int32)
    folded = (index[None, :] * generator[:, None]) % modulus
    phase = folded.astype(jnp.float32) / modulus + shift[:, None]
    return jnp.sin(2.0 * jnp.pi * phase)


def cost_block(points, targets):
    cross = lax.dot_general(points, targets, (((0,), (0,)), ((), ())), precision=highest, preferred_element_type=jnp.float32)
    near = 0.5 * jnp.sum(points * points, 0)
    far = 0.5 * jnp.sum(targets * targets, 0)
    return near[:, None] + far[None, :] - cross


def reference(generator, shift, targets, log_weights):
    peak = jnp.max(log_weights)
    log_b = log_weights - (peak + jnp.log(jnp.sum(jnp.exp(log_weights - peak))))
    log_a = -math.log(NS)
    block = min(512, NS)
    count = NS // block
    potential_g = jnp.zeros((NT,), jnp.float32)
    potential_f = jnp.zeros((NS,), jnp.float32)
    for step in range(ITERS):
        def row_pass(index, current_g=potential_g):
            points = lattice_block(generator, shift, index * block, block, NS)
            scores = log_b[None, :] + (current_g[None, :] - cost_block(points, targets)) / blur_level
            top = jnp.max(scores, 1)
            return -blur_level * (top + jnp.log(jnp.sum(jnp.exp(scores - top[:, None]), 1)))

        potential_f = lax.map(row_pass, jnp.arange(count, dtype=jnp.int32)).reshape(NS)

        def column_pass(carry, index, current_f=potential_f):
            peak_c, total_c = carry
            start = index * block
            points = lattice_block(generator, shift, start, block, NS)
            part = lax.dynamic_slice_in_dim(current_f, start, block)
            scores = log_a + (part[:, None] - cost_block(points, targets)) / blur_level
            top = jnp.maximum(peak_c, jnp.max(scores, 0))
            total = total_c * jnp.exp(peak_c - top) + jnp.sum(jnp.exp(scores - top[None, :]), 0)
            return (top, total), None

        start_carry = (jnp.full((NT,), -1e30, jnp.float32), jnp.zeros((NT,), jnp.float32))
        (top, total), unused = lax.scan(column_pass, start_carry, jnp.arange(count, dtype=jnp.int32))
        potential_g = -blur_level * (top + jnp.log(total))
    return potential_f, potential_g
```

```python
import math
import jax
import jax.numpy as jnp
from jax import lax
from jax.experimental import pallas as pl
from jax.experimental.pallas import tpu as pltpu
from jax.sharding import PartitionSpec as P

DIM = 64
NSRC = 2048
NTGT = 1024
LANES = 128
SRC_TILES = NSRC // LANES
TGT_TILES = NTGT // LANES
BLUR = 0.1
LOG2E = 1.4426950408889634
KAPPA = LOG2E / BLUR
UNKAPPA = 1.0 / KAPPA
WIDTH = 256
f32 = jnp.float32
bf16 = jnp.bfloat16

SINE = (6.28318530707259, -41.34170211699658, 81.6052262062997, -76.7042813207251, 42.00980570831026, -14.394135222236105)


def split(x):
    hi = x.astype(bf16)
    lo = (x - hi.astype(f32)).astype(bf16)
    return hi, lo


def pieces(x):
    first = x.astype(bf16).astype(f32)
    rest = x - first
    second = rest.astype(bf16).astype(f32)
    return first, second, rest - second


def column_of(values, kind):
    sub = lax.broadcasted_iota(jnp.int32, (8, LANES), 0)
    groups = []
    for g in range(DIM // 8):
        v = jnp.full((8, LANES), values[8 * g], kind)
        for s in range(1, 8):
            v = jnp.where(sub == s, values[8 * g + s], v)
        groups.append(v)
    return jnp.concatenate(groups, 0)


def sine_turns(u):
    r = u - jnp.floor(u + 0.5)
    a = jnp.abs(r)
    b = jnp.minimum(a, 0.5 - a)
    z = b * b
    p = jnp.full_like(z, SINE[-1])
    for c in SINE[-2::-1]:
        p = p * z + c
    v = b * p
    return jnp.where(r < 0, -v, v)


def place_terms(a_ref, d_ref, rows, tiles):
    d_ref[...] = jnp.zeros_like(d_ref)
    for k, piece in enumerate(pieces(rows)):
        d_ref[:, k, :] = piece
    for t in range(tiles):
        a_ref[LANES * t : LANES * (t + 1), LANES : LANES + 8] = d_ref[t].T.astype(bf16)


def fill_left(a_ref, half):
    lane = lax.broadcasted_iota(jnp.int32, half.shape, 1)
    a_ref[:, :LANES] = half
    a_ref[:, LANES:] = jnp.where(lane < 64, jnp.zeros_like(half), half)


def log_sums(a_ref, b_ref, out):
    count = b_ref.shape[1] // WIDTH

    for n in range(count):
        s = jnp.dot(a_ref[...], b_ref[:, WIDTH * n : WIDTH * (n + 1)], preferred_element_type=f32)
        top = jnp.max(s, 0, keepdims=True)
        row = top + jnp.log2(jnp.sum(jnp.exp2(s - top), 0, keepdims=True))
        for k in range(WIDTH // LANES):
            r = n * (WIDTH // LANES) + k
            out[r : r + 1, :] = row[:, LANES * k : LANES * (k + 1)]


def merged(parts):
    top = jnp.max(parts, 0)
    return top + jnp.log2(jnp.sum(jnp.exp2(parts - top[None]), 0))


def ones_rows():
    row = lax.broadcasted_iota(jnp.int32, (64, LANES), 0)
    return jnp.where(row < 3, 1.0, 0.0).astype(bf16)


def first_rows(gen, shift, t_ref, w_ref, half_ref, b_ref, c_ref, far_ref, near_ref, out_ref, a_ref, d_ref, l_ref):
    offset = lax.axis_index("src") * NSRC
    modulus = NSRC * lax.axis_size("src")
    g = column_of(gen, jnp.int32)
    sh = column_of(shift, f32)
    lane = lax.broadcasted_iota(jnp.int32, (DIM, LANES), 1)
    phase = ((offset + lane) * g) & (modulus - 1)
    step = (LANES * g) & (modulus - 1)
    ones = ones_rows()
    for t in range(SRC_TILES):
        cols = slice(LANES * t, LANES * (t + 1))
        points = sine_turns(phase.astype(f32) * (1.0 / modulus) + sh)
        near_ref[t : t + 1, :] = 0.5 * jnp.sum(points * points, 0, keepdims=True)
        hi, lo = split(points * KAPPA)
        b_ref[0:64, cols] = hi
        b_ref[64:128, cols] = hi
        b_ref[128:192, cols] = ones
        b_ref[192:256, cols] = lo
        phase = (phase + step) & (modulus - 1)
    w = w_ref[...] * LOG2E
    c_ref[...] = w
    for t in range(TGT_TILES):
        rows = slice(LANES * t, LANES * (t + 1))
        y = t_ref[:, rows]
        far_ref[t : t + 1, :] = 0.5 * jnp.sum(y * y, 0, keepdims=True)
        hi = y.astype(bf16).astype(f32)
        half_ref[rows, :] = jnp.concatenate([y - hi, hi], 0).T.astype(bf16)
    fill_left(a_ref, half_ref[...])
    place_terms(a_ref, d_ref, w - KAPPA * far_ref[...], TGT_TILES)
    top = jnp.max(w, keepdims=True)
    total = top + jnp.log2(jnp.sum(jnp.exp2(w - top), keepdims=True))
    l_ref[SRC_TILES:, :] = jnp.broadcast_to(total, (8, LANES))
    log_sums(a_ref, b_ref, l_ref)
    out_ref[...] = jnp.broadcast_to(l_ref[...][None], out_ref.shape)


def source_side(b_ref, t_ref, half_ref, out_ref):
    for t in range(SRC_TILES):
        cols = slice(LANES * t, LANES * (t + 1))
        both = jnp.concatenate([b_ref[192:256, cols], b_ref[0:64, cols]], 0).astype(f32)
        half_ref[cols, :] = both.T.astype(bf16)
    ones = ones_rows()
    for t in range(TGT_TILES):
        cols = slice(LANES * t, LANES * (t + 1))
        hi, lo = split(t_ref[:, cols])
        out_ref[0:64, cols] = hi
        out_ref[64:128, cols] = hi
        out_ref[128:192, cols] = ones
        out_ref[192:256, cols] = lo


def first_columns(parts_ref, half_ref, b_ref, norm_ref, out_ref, a_ref, d_ref, l_ref):
    every = merged(parts_ref[...])
    norm = every[SRC_TILES:, :]
    norm_ref[...] = norm
    rows = (norm[0:1, :] - every[:SRC_TILES, :]) - math.log2(NSRC * lax.axis_size("src"))
    fill_left(a_ref, half_ref[...])
    place_terms(a_ref, d_ref, rows, SRC_TILES)
    log_sums(a_ref, b_ref, l_ref)
    out_ref[...] = jnp.broadcast_to(l_ref[...][None], out_ref.shape)


def later_rows(parts_ref, half_ref, b_ref, c_ref, out_ref, a_ref, d_ref, l_ref):
    rows = c_ref[...] - merged(parts_ref[...])
    fill_left(a_ref, half_ref[...])
    place_terms(a_ref, d_ref, rows, TGT_TILES)
    log_sums(a_ref, b_ref, l_ref)
    out_ref[...] = jnp.broadcast_to(l_ref[...][None], out_ref.shape)


def later_columns(parts_ref, half_ref, b_ref, norm_ref, near_ref, f_ref, out_ref, a_ref, d_ref, l_ref):
    every = merged(parts_ref[...]) - norm_ref[0:1, :]
    f_ref[...] = near_ref[...] - UNKAPPA * every
    fill_left(a_ref, half_ref[...])
    place_terms(a_ref, d_ref, -math.log2(NSRC * lax.axis_size("src")) - every, SRC_TILES)
    log_sums(a_ref, b_ref, l_ref)
    out_ref[...] = jnp.broadcast_to(l_ref[...][None], out_ref.shape)


def last_columns(parts_ref, far_ref, g_ref):
    g_ref[...] = far_ref[...] - UNKAPPA * merged(parts_ref[...])


def shape(dims, kind=f32):
    return jax.ShapeDtypeStruct(dims, kind)


def call(body, outs, inputs, scratch=(), smem=0):
    specs = [pl.BlockSpec(memory_space=pltpu.SMEM)] * smem
    specs += [pl.BlockSpec(memory_space=pltpu.VMEM)] * (len(inputs) - smem)
    return pl.pallas_call(
        body,
        out_shape=outs,
        in_specs=specs,
        out_specs=jax.tree.map(lambda _: pl.BlockSpec(memory_space=pltpu.VMEM), outs),
        scratch_shapes=scratch,
        name=body.__name__,
    )(*inputs)


def exchanged(x, axis):
    return lax.all_to_all(x, axis, split_axis=0, concat_axis=0, tiled=True)


def local(generator, shift, targets, log_weights):
    n_src, n_tgt = lax.axis_size("src"), lax.axis_size("tgt")
    f_tmp = lambda rows: [
        pltpu.VMEM((NTGT, 256), bf16),
        pltpu.VMEM((TGT_TILES, 8, LANES), f32),
        pltpu.VMEM((rows, LANES), f32),
    ]
    g_tmp = [
        pltpu.VMEM((NSRC, 256), bf16),
        pltpu.VMEM((SRC_TILES, 8, LANES), f32),
        pltpu.VMEM((TGT_TILES, LANES), f32),
    ]
    w = log_weights.reshape(TGT_TILES, LANES)
    f_half, f_right, c, far, near, part = call(
        first_rows,
        (
            shape((NTGT, LANES), bf16),
            shape((256, NSRC), bf16),
            shape((TGT_TILES, LANES)),
            shape((TGT_TILES, LANES)),
            shape((SRC_TILES, LANES)),
            shape((n_tgt, SRC_TILES + 8, LANES)),
        ),
        (generator, shift, targets, w),
        f_tmp(SRC_TILES + 8),
        smem=2,
    )
    got = exchanged(part, "tgt")
    g_half, g_right = call(
        source_side, (shape((NSRC, LANES), bf16), shape((256, NTGT), bf16)), (f_right, targets)
    )
    norm, part = call(
        first_columns,
        (shape((8, LANES)), shape((n_src, TGT_TILES, LANES))),
        (got, g_half, g_right),
        g_tmp,
    )
    got = exchanged(part, "src")
    part = call(
        later_rows, shape((n_tgt, SRC_TILES, LANES)), (got, f_half, f_right, c), f_tmp(SRC_TILES)
    )
    got = exchanged(part, "tgt")
    f, part = call(
        later_columns,
        (shape((SRC_TILES, LANES)), shape((n_src, TGT_TILES, LANES))),
        (got, g_half, g_right, norm, near),
        g_tmp,
    )
    got = exchanged(part, "src")
    g = call(last_columns, shape((TGT_TILES, LANES)), (got, far))
    return f.reshape(NSRC), g.reshape(NTGT)


def solution(mesh):
    in_specs = (P(), P(), P(None, "tgt"), P("tgt"))
    out_specs = (P("src"), P("tgt"))
    return jax.shard_map(local, mesh=mesh, in_specs=in_specs, out_specs=out_specs, check_vma=False)
```

```python
import math
import jax
import jax.numpy as jnp
from jax import lax
from jax.experimental import pallas as pl
from jax.experimental.pallas import tpu as pltpu
from jax.sharding import PartitionSpec as P

DIM = 64
NSRC = 2048
NTGT = 1024
LANES = 128
SRC_TILES = NSRC // LANES
TGT_TILES = NTGT // LANES
BLUR = 0.1
LOG2E = 1.4426950408889634
KAPPA = LOG2E / BLUR
UNKAPPA = 1.0 / KAPPA
WIDTH = 256
GRANT = 16 * 2**20
f32 = jnp.float32
bf16 = jnp.bfloat16

SINE = (6.28318530707259, -41.34170211699658, 81.6052262062997, -76.7042813207251, 42.00980570831026, -14.394135222236105)


def split(x):
    hi = x.astype(bf16)
    lo = (x - hi.astype(f32)).astype(bf16)
    return hi, lo


def pieces(x):
    first = x.astype(bf16).astype(f32)
    rest = x - first
    second = rest.astype(bf16).astype(f32)
    return first, second, rest - second


def column_of(values, kind):
    sub = lax.broadcasted_iota(jnp.int32, (8, LANES), 0)
    groups = []
    for g in range(DIM // 8):
        v = jnp.full((8, LANES), values[8 * g], kind)
        for s in range(1, 8):
            v = jnp.where(sub == s, values[8 * g + s], v)
        groups.append(v)
    return jnp.concatenate(groups, 0)


def sine_turns(u):
    r = u - jnp.floor(u + 0.5)
    a = jnp.abs(r)
    b = jnp.minimum(a, 0.5 - a)
    z = b * b
    p = jnp.full_like(z, SINE[-1])
    for c in SINE[-2::-1]:
        p = p * z + c
    v = b * p
    return jnp.where(r < 0, -v, v)


def place_terms(a_ref, d_ref, rows, tiles):
    d_ref[...] = jnp.zeros_like(d_ref)
    for k, piece in enumerate(pieces(rows)):
        d_ref[:, k, :] = piece
    for t in range(tiles):
        a_ref[LANES * t : LANES * (t + 1), LANES : LANES + 8] = d_ref[t].T.astype(bf16)


def fill_left(a_ref, half):
    lane = lax.broadcasted_iota(jnp.int32, half.shape, 1)
    a_ref[:, :LANES] = half
    a_ref[:, LANES:] = jnp.where(lane < 64, jnp.zeros_like(half), half)


def log_sums(a_ref, b_ref, out):
    count = b_ref.shape[1] // WIDTH

    for n in range(count):
        s = jnp.dot(a_ref[...], b_ref[:, WIDTH * n : WIDTH * (n + 1)], preferred_element_type=f32)
        top = jnp.max(s, 0, keepdims=True)
        row = top + jnp.log2(jnp.sum(jnp.exp2(s - top), 0, keepdims=True))
        for k in range(WIDTH // LANES):
            r = n * (WIDTH // LANES) + k
            out[r : r + 1, :] = row[:, LANES * k : LANES * (k + 1)]


def merged(parts):
    top = jnp.max(parts, 0)
    return top + jnp.log2(jnp.sum(jnp.exp2(parts - top[None]), 0))


def ones_rows():
    row = lax.broadcasted_iota(jnp.int32, (64, LANES), 0)
    return jnp.where(row < 3, 1.0, 0.0).astype(bf16)


def first_rows(gen, shift, t_ref, w_ref, half_ref, b_ref, c_ref, far_ref, near_ref, out_ref, a_ref, d_ref, l_ref):
    offset = lax.axis_index("src") * NSRC
    modulus = NSRC * lax.axis_size("src")
    g = column_of(gen, jnp.int32)
    sh = column_of(shift, f32)
    lane = lax.broadcasted_iota(jnp.int32, (DIM, LANES), 1)
    phase = ((offset + lane) * g) & (modulus - 1)
    step = (LANES * g) & (modulus - 1)
    ones = ones_rows()
    for t in range(SRC_TILES):
        cols = slice(LANES * t, LANES * (t + 1))
        points = sine_turns(phase.astype(f32) * (1.0 / modulus) + sh)
        near_ref[t : t + 1, :] = 0.5 * jnp.sum(points * points, 0, keepdims=True)
        hi, lo = split(points * KAPPA)
        b_ref[0:64, cols] = hi
        b_ref[64:128, cols] = hi
        b_ref[128:192, cols] = ones
        b_ref[192:256, cols] = lo
        phase = (phase + step) & (modulus - 1)
    w = w_ref[...] * LOG2E
    c_ref[...] = w
    for t in range(TGT_TILES):
        rows = slice(LANES * t, LANES * (t + 1))
        y = t_ref[:, rows]
        far_ref[t : t + 1, :] = 0.5 * jnp.sum(y * y, 0, keepdims=True)
        hi = y.astype(bf16).astype(f32)
        half_ref[rows, :] = jnp.concatenate([y - hi, hi], 0).T.astype(bf16)
    fill_left(a_ref, half_ref[...])
    place_terms(a_ref, d_ref, w - KAPPA * far_ref[...], TGT_TILES)
    top = jnp.max(w, keepdims=True)
    total = top + jnp.log2(jnp.sum(jnp.exp2(w - top), keepdims=True))
    l_ref[SRC_TILES:, :] = jnp.broadcast_to(total, (8, LANES))
    log_sums(a_ref, b_ref, l_ref)
    out_ref[...] = jnp.broadcast_to(l_ref[...][None], out_ref.shape)


def source_side(b_ref, t_ref, half_ref, out_ref):
    for t in range(SRC_TILES):
        cols = slice(LANES * t, LANES * (t + 1))
        both = jnp.concatenate([b_ref[192:256, cols], b_ref[0:64, cols]], 0).astype(f32)
        half_ref[cols, :] = both.T.astype(bf16)
    ones = ones_rows()
    for t in range(TGT_TILES):
        cols = slice(LANES * t, LANES * (t + 1))
        hi, lo = split(t_ref[:, cols])
        out_ref[0:64, cols] = hi
        out_ref[64:128, cols] = hi
        out_ref[128:192, cols] = ones
        out_ref[192:256, cols] = lo


def first_columns(parts_ref, half_ref, b_ref, norm_ref, out_ref, a_ref, d_ref, l_ref):
    every = merged(parts_ref[...])
    norm = every[SRC_TILES:, :]
    norm_ref[...] = norm
    rows = (norm[0:1, :] - every[:SRC_TILES, :]) - math.log2(NSRC * lax.axis_size("src"))
    fill_left(a_ref, half_ref[...])
    place_terms(a_ref, d_ref, rows, SRC_TILES)
    log_sums(a_ref, b_ref, l_ref)
    out_ref[...] = jnp.broadcast_to(l_ref[...][None], out_ref.shape)


def later_rows(parts_ref, half_ref, b_ref, c_ref, out_ref, a_ref, d_ref, l_ref):
    rows = c_ref[...] - merged(parts_ref[...])
    fill_left(a_ref, half_ref[...])
    place_terms(a_ref, d_ref, rows, TGT_TILES)
    log_sums(a_ref, b_ref, l_ref)
    out_ref[...] = jnp.broadcast_to(l_ref[...][None], out_ref.shape)


def later_columns(parts_ref, half_ref, b_ref, norm_ref, near_ref, f_ref, out_ref, a_ref, d_ref, l_ref):
    every = merged(parts_ref[...]) - norm_ref[0:1, :]
    f_ref[...] = near_ref[...] - UNKAPPA * every
    fill_left(a_ref, half_ref[...])
    place_terms(a_ref, d_ref, -math.log2(NSRC * lax.axis_size("src")) - every, SRC_TILES)
    log_sums(a_ref, b_ref, l_ref)
    out_ref[...] = jnp.broadcast_to(l_ref[...][None], out_ref.shape)


def last_columns(parts_ref, far_ref, g_ref):
    g_ref[...] = far_ref[...] - UNKAPPA * merged(parts_ref[...])


def shape(dims, kind=f32):
    return jax.ShapeDtypeStruct(dims, kind)


def call(body, outs, inputs, scratch=(), smem=0):
    specs = [pl.BlockSpec(memory_space=pltpu.SMEM)] * smem
    specs += [pl.BlockSpec(memory_space=pltpu.VMEM)] * (len(inputs) - smem)
    return pl.pallas_call(
        body,
        out_shape=outs,
        in_specs=specs,
        out_specs=jax.tree.map(lambda _: pl.BlockSpec(memory_space=pltpu.VMEM), outs),
        scratch_shapes=scratch,
        name=body.__name__,
        compiler_params=pltpu.CompilerParams(vmem_limit_bytes=GRANT),
    )(*inputs)


def exchanged(x, axis):
    return lax.all_to_all(x, axis, split_axis=0, concat_axis=0, tiled=True)


def local(generator, shift, targets, log_weights):
    n_src, n_tgt = lax.axis_size("src"), lax.axis_size("tgt")
    f_tmp = lambda rows: [
        pltpu.VMEM((NTGT, 256), bf16),
        pltpu.VMEM((TGT_TILES, 8, LANES), f32),
        pltpu.VMEM((rows, LANES), f32),
    ]
    g_tmp = [
        pltpu.VMEM((NSRC, 256), bf16),
        pltpu.VMEM((SRC_TILES, 8, LANES), f32),
        pltpu.VMEM((TGT_TILES, LANES), f32),
    ]
    w = log_weights.reshape(TGT_TILES, LANES)
    f_half, f_right, c, far, near, part = call(
        first_rows,
        (
            shape((NTGT, LANES), bf16),
            shape((256, NSRC), bf16),
            shape((TGT_TILES, LANES)),
            shape((TGT_TILES, LANES)),
            shape((SRC_TILES, LANES)),
            shape((n_tgt, SRC_TILES + 8, LANES)),
        ),
        (generator, shift, targets, w),
        f_tmp(SRC_TILES + 8),
        smem=2,
    )
    got = exchanged(part, "tgt")
    g_half, g_right = call(
        source_side, (shape((NSRC, LANES), bf16), shape((256, NTGT), bf16)), (f_right, targets)
    )
    norm, part = call(
        first_columns,
        (shape((8, LANES)), shape((n_src, TGT_TILES, LANES))),
        (got, g_half, g_right),
        g_tmp,
    )
    got = exchanged(part, "src")
    part = call(
        later_rows, shape((n_tgt, SRC_TILES, LANES)), (got, f_half, f_right, c), f_tmp(SRC_TILES)
    )
    got = exchanged(part, "tgt")
    f, part = call(
        later_columns,
        (shape((SRC_TILES, LANES)), shape((n_src, TGT_TILES, LANES))),
        (got, g_half, g_right, norm, near),
        g_tmp,
    )
    got = exchanged(part, "src")
    g = call(last_columns, shape((TGT_TILES, LANES)), (got, far))
    return f.reshape(NSRC), g.reshape(NTGT)


def solution(mesh):
    in_specs = (P(), P(), P(None, "tgt"), P("tgt"))
    out_specs = (P("src"), P("tgt"))
    return jax.shard_map(local, mesh=mesh, in_specs=in_specs, out_specs=out_specs, check_vma=False)
```

```python
import math
import jax
import jax.numpy as jnp
from jax import lax
from jax.experimental import pallas as pl
from jax.experimental.pallas import tpu as pltpu
from jax.sharding import PartitionSpec as P

DIM = 64
NSRC = 2048
NTGT = 1024
LANES = 128
SRC_TILES = NSRC // LANES
TGT_TILES = NTGT // LANES
BLUR = 0.1
LOG2E = 1.4426950408889634
KAPPA = LOG2E / BLUR
UNKAPPA = 1.0 / KAPPA
WIDTH = 256
ROWS = 64
GRANT = 16 * 2**20
f32 = jnp.float32
bf16 = jnp.bfloat16

SINE = (6.28318530707259, -41.34170211699658, 81.6052262062997, -76.7042813207251, 42.00980570831026, -14.394135222236105)


def split(x):
    hi = x.astype(bf16)
    lo = (x - hi.astype(f32)).astype(bf16)
    return hi, lo


def pieces(x):
    first = x.astype(bf16).astype(f32)
    rest = x - first
    second = rest.astype(bf16).astype(f32)
    return first, second, rest - second


def column_of(values, kind):
    sub = lax.broadcasted_iota(jnp.int32, (8, LANES), 0)
    groups = []
    for g in range(DIM // 8):
        v = jnp.full((8, LANES), values[8 * g], kind)
        for s in range(1, 8):
            v = jnp.where(sub == s, values[8 * g + s], v)
        groups.append(v)
    return jnp.concatenate(groups, 0)


def sine_turns(u):
    r = u - jnp.floor(u + 0.5)
    a = jnp.abs(r)
    b = jnp.minimum(a, 0.5 - a)
    z = b * b
    p = jnp.full_like(z, SINE[-1])
    for c in SINE[-2::-1]:
        p = p * z + c
    v = b * p
    return jnp.where(r < 0, -v, v)


def place_terms(a_ref, d_ref, rows, tiles):
    d_ref[...] = jnp.zeros_like(d_ref)
    for k, piece in enumerate(pieces(rows)):
        d_ref[:, k, :] = piece
    for t in range(tiles):
        a_ref[LANES * t : LANES * (t + 1), LANES : LANES + 8] = d_ref[t].T.astype(bf16)


def fill_left(a_ref, half):
    lane = lax.broadcasted_iota(jnp.int32, half.shape, 1)
    a_ref[:, :LANES] = half
    a_ref[:, LANES:] = jnp.where(lane < 64, jnp.zeros_like(half), half)


def log_sums(a_ref, b_ref, out):
    for n in range(b_ref.shape[1] // WIDTH):
        s = jnp.dot(a_ref[...], b_ref[:, WIDTH * n : WIDTH * (n + 1)], preferred_element_type=f32)
        found = [([], []) for _ in range(WIDTH // LANES)]
        for m in range(0, s.shape[0], ROWS):
            for k, (tops, sums) in enumerate(found):
                block = s[m : m + ROWS, LANES * k : LANES * (k + 1)].reshape(ROWS // 8, 8, LANES)
                top = jnp.max(block, 0)
                tops.append(top)
                sums.append(jnp.sum(jnp.exp2(block - top[None]), 0))
        for k, (tops, sums) in enumerate(found):
            tops, sums = jnp.concatenate(tops, 0), jnp.concatenate(sums, 0)
            top = jnp.max(tops, 0, keepdims=True)
            r = n * (WIDTH // LANES) + k
            out[r : r + 1, :] = top + jnp.log2(jnp.sum(sums * jnp.exp2(tops - top), 0, keepdims=True))


def merged(parts):
    top = jnp.max(parts, 0)
    return top + jnp.log2(jnp.sum(jnp.exp2(parts - top[None]), 0))


def ones_rows():
    row = lax.broadcasted_iota(jnp.int32, (64, LANES), 0)
    return jnp.where(row < 3, 1.0, 0.0).astype(bf16)


def first_rows(
    gen_hbm, shift_hbm, t_hbm, w_hbm,
    half_ref, b_ref, g_half_ref, g_b_ref, c_ref, far_ref, near_ref, out_ref,
    a_ref, d_ref, l_ref, gen, shift, t_ref, w_ref, sems,
):
    moves = [
        pltpu.make_async_copy(src, dst, sems.at[k])
        for k, (src, dst) in enumerate(
            ((gen_hbm, gen), (shift_hbm, shift), (t_hbm, t_ref), (w_hbm, w_ref))
        )
    ]
    for move in moves:
        move.start()
    ones = ones_rows()
    offset = lax.axis_index("src") * NSRC
    modulus = NSRC * lax.axis_size("src")
    moves[0].wait()
    moves[1].wait()
    g = column_of(gen, jnp.int32)
    sh = column_of(shift, f32)
    lane = lax.broadcasted_iota(jnp.int32, (DIM, LANES), 1)
    phase = ((offset + lane) * g) & (modulus - 1)
    step = (LANES * g) & (modulus - 1)
    for t in range(SRC_TILES):
        cols = slice(LANES * t, LANES * (t + 1))
        points = sine_turns(phase.astype(f32) * (1.0 / modulus) + sh)
        near_ref[t : t + 1, :] = 0.5 * jnp.sum(points * points, 0, keepdims=True)
        scaled = points * KAPPA
        hi = scaled.astype(bf16).astype(f32)
        lo = scaled - hi
        b_ref[0:64, cols] = hi.astype(bf16)
        b_ref[64:128, cols] = hi.astype(bf16)
        b_ref[128:192, cols] = ones
        b_ref[192:256, cols] = lo.astype(bf16)
        g_half_ref[cols, :] = jnp.concatenate([lo, hi], 0).T.astype(bf16)
        phase = (phase + step) & (modulus - 1)
    moves[2].wait()
    moves[3].wait()
    w = w_ref[...] * LOG2E
    c_ref[...] = w
    for t in range(TGT_TILES):
        rows = slice(LANES * t, LANES * (t + 1))
        y = t_ref[:, rows]
        far_ref[t : t + 1, :] = 0.5 * jnp.sum(y * y, 0, keepdims=True)
        hi = y.astype(bf16).astype(f32)
        half_ref[rows, :] = jnp.concatenate([y - hi, hi], 0).T.astype(bf16)
        g_b_ref[0:64, rows] = hi.astype(bf16)
        g_b_ref[64:128, rows] = hi.astype(bf16)
        g_b_ref[128:192, rows] = ones
        g_b_ref[192:256, rows] = (y - hi).astype(bf16)
    fill_left(a_ref, half_ref[...])
    place_terms(a_ref, d_ref, w - KAPPA * far_ref[...], TGT_TILES)
    top = jnp.max(w, keepdims=True)
    total = top + jnp.log2(jnp.sum(jnp.exp2(w - top), keepdims=True))
    log_sums(a_ref, b_ref, l_ref)
    l_ref[SRC_TILES:, :] = jnp.broadcast_to(total, (8, LANES))
    for t in range(SRC_TILES + 1):
        row = jnp.broadcast_to(l_ref[t : t + 1, :], (out_ref.shape[0], LANES))
        out_ref[:, 0, LANES * t : LANES * (t + 1)] = row


def first_columns(parts_ref, half_ref, b_ref, norm_ref, out_ref, a_ref, d_ref, l_ref):
    every = []
    for t in range(SRC_TILES + 1):
        parts = parts_ref[:, 0, LANES * t : LANES * (t + 1)]
        top = jnp.max(parts, 0, keepdims=True)
        every.append(top + jnp.log2(jnp.sum(jnp.exp2(parts - top), 0, keepdims=True)))
    norm_ref[...] = jnp.broadcast_to(every[-1], norm_ref.shape)
    rows = (every[-1] - jnp.concatenate(every[:-1], 0)) - math.log2(NSRC * lax.axis_size("src"))
    fill_left(a_ref, half_ref[...])
    place_terms(a_ref, d_ref, rows, SRC_TILES)
    log_sums(a_ref, b_ref, l_ref)
    out_ref[...] = jnp.broadcast_to(l_ref[...][None], out_ref.shape)


def later_rows(parts_ref, half_ref, b_ref, c_ref, out_ref, a_ref, d_ref, l_ref):
    rows = c_ref[...] - merged(parts_ref[...])
    fill_left(a_ref, half_ref[...])
    place_terms(a_ref, d_ref, rows, TGT_TILES)
    log_sums(a_ref, b_ref, l_ref)
    out_ref[...] = jnp.broadcast_to(l_ref[...][None], out_ref.shape)


def later_columns(parts_ref, half_ref, b_ref, norm_ref, near_ref, f_ref, out_ref, a_ref, d_ref, l_ref):
    every = merged(parts_ref[...]) - norm_ref[0:1, :]
    f_ref[...] = near_ref[...] - UNKAPPA * every
    fill_left(a_ref, half_ref[...])
    place_terms(a_ref, d_ref, -math.log2(NSRC * lax.axis_size("src")) - every, SRC_TILES)
    log_sums(a_ref, b_ref, l_ref)
    out_ref[...] = jnp.broadcast_to(l_ref[...][None], out_ref.shape)


def last_columns(parts_ref, far_ref, g_ref):
    g_ref[...] = far_ref[...] - UNKAPPA * merged(parts_ref[...])


def shape(dims, kind=f32):
    return jax.ShapeDtypeStruct(dims, kind)


def call(body, outs, inputs, scratch=(), space=pltpu.VMEM):
    return pl.pallas_call(
        body,
        out_shape=outs,
        in_specs=[pl.BlockSpec(memory_space=space)] * len(inputs),
        out_specs=jax.tree.map(lambda _: pl.BlockSpec(memory_space=pltpu.VMEM), outs),
        scratch_shapes=scratch,
        name=body.__name__,
        compiler_params=pltpu.CompilerParams(vmem_limit_bytes=GRANT),
    )(*inputs)


def exchanged(x, axis):
    return lax.all_to_all(x, axis, split_axis=0, concat_axis=0, tiled=True)


def local(generator, shift, targets, log_weights):
    n_src, n_tgt = lax.axis_size("src"), lax.axis_size("tgt")
    f_tmp = lambda rows: [
        pltpu.VMEM((NTGT, 256), bf16),
        pltpu.VMEM((TGT_TILES, 8, LANES), f32),
        pltpu.VMEM((rows, LANES), f32),
    ]
    g_tmp = [
        pltpu.VMEM((NSRC, 256), bf16),
        pltpu.VMEM((SRC_TILES, 8, LANES), f32),
        pltpu.VMEM((TGT_TILES, LANES), f32),
    ]
    w = log_weights.reshape(TGT_TILES, LANES)
    f_half, f_right, g_half, g_right, c, far, near, part = call(
        first_rows,
        (
            shape((NTGT, LANES), bf16),
            shape((256, NSRC), bf16),
            shape((NSRC, LANES), bf16),
            shape((256, NTGT), bf16),
            shape((TGT_TILES, LANES)),
            shape((TGT_TILES, LANES)),
            shape((SRC_TILES, LANES)),
            shape((n_tgt, 1, (SRC_TILES + 1) * LANES)),
        ),
        (generator, shift, targets, w),
        f_tmp(SRC_TILES + 8)
        + [
            pltpu.SMEM((DIM,), jnp.int32),
            pltpu.SMEM((DIM,), f32),
            pltpu.VMEM((DIM, NTGT), f32),
            pltpu.VMEM((TGT_TILES, LANES), f32),
            pltpu.SemaphoreType.DMA((4,)),
        ],
        space=pltpu.HBM,
    )
    got = exchanged(part, "tgt")
    norm, part = call(
        first_columns,
        (shape((8, LANES)), shape((n_src, TGT_TILES, LANES))),
        (got, g_half, g_right),
        g_tmp,
    )
    got = exchanged(part, "src")
    part = call(
        later_rows, shape((n_tgt, SRC_TILES, LANES)), (got, f_half, f_right, c), f_tmp(SRC_TILES)
    )
    got = exchanged(part, "tgt")
    f, part = call(
        later_columns,
        (shape((SRC_TILES, LANES)), shape((n_src, TGT_TILES, LANES))),
        (got, g_half, g_right, norm, near),
        g_tmp,
    )
    got = exchanged(part, "src")
    g = call(last_columns, shape((TGT_TILES, LANES)), (got, far))
    return f.reshape(NSRC), g.reshape(NTGT)


def solution(mesh):
    in_specs = (P(), P(), P(None, "tgt"), P("tgt"))
    out_specs = (P("src"), P("tgt"))
    return jax.shard_map(local, mesh=mesh, in_specs=in_specs, out_specs=out_specs, check_vma=False)
```

```python
import math
import jax
import jax.numpy as jnp
from jax import lax
from jax.experimental import pallas as pl
from jax.experimental.pallas import tpu as pltpu
from jax.sharding import PartitionSpec as P

DIM = 64
NSRC = 2048
NTGT = 1024
LANES = 128
SRC_TILES = NSRC // LANES
TGT_TILES = NTGT // LANES
BLUR = 0.1
LOG2E = 1.4426950408889634
KAPPA = LOG2E / BLUR
UNKAPPA = 1.0 / KAPPA
WIDTH = 256
ROWS = 64
GRANT = 16 * 2**20
f32 = jnp.float32
bf16 = jnp.bfloat16

SINE = (6.28318530707259, -41.34170211699658, 81.6052262062997, -76.7042813207251, 42.00980570831026, -14.394135222236105)


def split(x):
    hi = x.astype(bf16)
    lo = (x - hi.astype(f32)).astype(bf16)
    return hi, lo


def pieces(x):
    first = x.astype(bf16).astype(f32)
    rest = x - first
    second = rest.astype(bf16).astype(f32)
    return first, second, rest - second


def column_of(values, kind):
    sub = lax.broadcasted_iota(jnp.int32, (8, LANES), 0)
    groups = []
    for g in range(DIM // 8):
        v = jnp.full((8, LANES), values[8 * g], kind)
        for s in range(1, 8):
            v = jnp.where(sub == s, values[8 * g + s], v)
        groups.append(v)
    return jnp.concatenate(groups, 0)


def sine_turns(u):
    r = u - jnp.floor(u + 0.5)
    a = jnp.abs(r)
    b = jnp.minimum(a, 0.5 - a)
    z = b * b
    p = jnp.full_like(z, SINE[-1])
    for c in SINE[-2::-1]:
        p = p * z + c
    v = b * p
    return jnp.where(r < 0, -v, v)


def place_terms(a_ref, d_ref, rows, tiles):
    d_ref[...] = jnp.zeros_like(d_ref)
    for k, piece in enumerate(pieces(rows)):
        d_ref[:, k, :] = piece
    for t in range(tiles):
        a_ref[LANES * t : LANES * (t + 1), LANES : LANES + 8] = d_ref[t].T.astype(bf16)


def fill_left(a_ref, half):
    lane = lax.broadcasted_iota(jnp.int32, half.shape, 1)
    a_ref[:, :LANES] = half
    a_ref[:, LANES:] = jnp.where(lane < 64, jnp.zeros_like(half), half)


def log_sums(a_ref, b_ref, out):
    for n in range(b_ref.shape[1] // WIDTH):
        s = jnp.dot(a_ref[...], b_ref[:, WIDTH * n : WIDTH * (n + 1)], preferred_element_type=f32)
        found = [([], []) for _ in range(WIDTH // LANES)]
        for m in range(0, s.shape[0], ROWS):
            for k, (tops, sums) in enumerate(found):
                block = s[m : m + ROWS, LANES * k : LANES * (k + 1)].reshape(ROWS // 8, 8, LANES)
                top = jnp.max(block, 0)
                tops.append(top)
                sums.append(jnp.sum(jnp.exp2(block - top[None]), 0))
        for k, (tops, sums) in enumerate(found):
            tops, sums = jnp.concatenate(tops, 0), jnp.concatenate(sums, 0)
            top = jnp.max(tops, 0, keepdims=True)
            r = n * (WIDTH // LANES) + k
            out[r : r + 1, :] = top + jnp.log2(jnp.sum(sums * jnp.exp2(tops - top), 0, keepdims=True))


def merged(parts):
    top = jnp.max(parts, 0)
    return top + jnp.log2(jnp.sum(jnp.exp2(parts - top[None]), 0))


def ones_rows():
    row = lax.broadcasted_iota(jnp.int32, (64, LANES), 0)
    return jnp.where(row < 3, 1.0, 0.0).astype(bf16)


def first_rows(
    gen_hbm, shift_hbm, t_hbm, w_hbm,
    half_ref, b_ref, g_half_ref, g_b_ref, c_ref, far_ref, near_ref, out_ref,
    a_ref, d_ref, l_ref, gen, shift, t_ref, w_ref, sems,
):
    moves = [
        pltpu.make_async_copy(src, dst, sems.at[k])
        for k, (src, dst) in enumerate(
            ((gen_hbm, gen), (shift_hbm, shift), (t_hbm, t_ref), (w_hbm, w_ref))
        )
    ]
    for move in moves:
        move.start()
    ones = ones_rows()
    offset = lax.axis_index("src") * NSRC
    modulus = NSRC * lax.axis_size("src")
    moves[0].wait()
    moves[1].wait()
    g = column_of(gen, jnp.int32)
    sh = column_of(shift, f32)
    lane = lax.broadcasted_iota(jnp.int32, (DIM, LANES), 1)
    phase = ((offset + lane) * g) & (modulus - 1)
    step = (LANES * g) & (modulus - 1)
    for t in range(SRC_TILES):
        cols = slice(LANES * t, LANES * (t + 1))
        points = sine_turns(phase.astype(f32) * (1.0 / modulus) + sh)
        near_ref[t : t + 1, :] = 0.5 * jnp.sum(points * points, 0, keepdims=True)
        scaled = points * KAPPA
        hi = scaled.astype(bf16).astype(f32)
        lo = scaled - hi
        b_ref[0:64, cols] = hi.astype(bf16)
        b_ref[64:128, cols] = hi.astype(bf16)
        b_ref[128:192, cols] = ones
        b_ref[192:256, cols] = lo.astype(bf16)
        g_half_ref[cols, :] = jnp.concatenate([lo, hi], 0).T.astype(bf16)
        phase = (phase + step) & (modulus - 1)
    moves[2].wait()
    moves[3].wait()
    w = w_ref[...] * LOG2E
    c_ref[...] = w
    for t in range(TGT_TILES):
        rows = slice(LANES * t, LANES * (t + 1))
        y = t_ref[:, rows]
        far_ref[t : t + 1, :] = 0.5 * jnp.sum(y * y, 0, keepdims=True)
        hi = y.astype(bf16).astype(f32)
        half_ref[rows, :] = jnp.concatenate([y - hi, hi], 0).T.astype(bf16)
        g_b_ref[0:64, rows] = hi.astype(bf16)
        g_b_ref[64:128, rows] = hi.astype(bf16)
        g_b_ref[128:192, rows] = ones
        g_b_ref[192:256, rows] = (y - hi).astype(bf16)
    fill_left(a_ref, half_ref[...])
    place_terms(a_ref, d_ref, w - KAPPA * far_ref[...], TGT_TILES)
    top = jnp.max(w, keepdims=True)
    total = top + jnp.log2(jnp.sum(jnp.exp2(w - top), keepdims=True))
    log_sums(a_ref, b_ref, l_ref)
    l_ref[SRC_TILES:, :] = jnp.broadcast_to(total, (8, LANES))
    for t in range(SRC_TILES + 1):
        row = jnp.broadcast_to(l_ref[t : t + 1, :], (out_ref.shape[0], LANES))
        out_ref[:, 0, LANES * t : LANES * (t + 1)] = row


def first_columns(parts_ref, half_ref, b_ref, norm_ref, out_ref, a_ref, d_ref, l_ref):
    every = []
    for t in range(SRC_TILES + 1):
        parts = parts_ref[:, 0, LANES * t : LANES * (t + 1)]
        top = jnp.max(parts, 0, keepdims=True)
        every.append(top + jnp.log2(jnp.sum(jnp.exp2(parts - top), 0, keepdims=True)))
    norm_ref[...] = jnp.broadcast_to(every[-1], norm_ref.shape)
    rows = (every[-1] - jnp.concatenate(every[:-1], 0)) - math.log2(NSRC * lax.axis_size("src"))
    fill_left(a_ref, half_ref[...])
    place_terms(a_ref, d_ref, rows, SRC_TILES)
    log_sums(a_ref, b_ref, l_ref)
    out_ref[...] = jnp.broadcast_to(l_ref[...][None], out_ref.shape)


def later_rows(parts_ref, half_ref, b_ref, c_ref, out_ref, a_ref, d_ref, l_ref):
    rows = c_ref[...] - merged(parts_ref[...])
    fill_left(a_ref, half_ref[...])
    place_terms(a_ref, d_ref, rows, TGT_TILES)
    log_sums(a_ref, b_ref, l_ref)
    out_ref[...] = jnp.broadcast_to(l_ref[...][None], out_ref.shape)


def later_columns(parts_ref, half_ref, b_ref, norm_ref, every_ref, out_ref, a_ref, d_ref, l_ref):
    every = merged(parts_ref[...]) - norm_ref[0:1, :]
    every_ref[...] = every
    fill_left(a_ref, half_ref[...])
    place_terms(a_ref, d_ref, -math.log2(NSRC * lax.axis_size("src")) - every, SRC_TILES)
    log_sums(a_ref, b_ref, l_ref)
    out_ref[...] = jnp.broadcast_to(l_ref[...][None], out_ref.shape)


def last_columns(parts_ref, far_ref, every_ref, near_ref, f_ref, g_ref):
    f_ref[...] = near_ref[...] - UNKAPPA * every_ref[...]
    g_ref[...] = far_ref[...] - UNKAPPA * merged(parts_ref[...])


def shape(dims, kind=f32):
    return jax.ShapeDtypeStruct(dims, kind)


def call(body, outs, inputs, scratch=(), space=pltpu.VMEM):
    if space is pltpu.HBM:
        inputs = [pltpu.with_memory_space_constraint(x, space) for x in inputs]
    return pl.pallas_call(
        body,
        out_shape=outs,
        in_specs=[pl.BlockSpec(memory_space=space)] * len(inputs),
        out_specs=jax.tree.map(lambda _: pl.BlockSpec(memory_space=pltpu.VMEM), outs),
        scratch_shapes=scratch,
        name=body.__name__,
        compiler_params=pltpu.CompilerParams(vmem_limit_bytes=GRANT),
    )(*inputs)


def exchanged(x, axis):
    return lax.all_to_all(x, axis, split_axis=0, concat_axis=0, tiled=True)


def local(generator, shift, targets, log_weights):
    n_src, n_tgt = lax.axis_size("src"), lax.axis_size("tgt")
    f_tmp = lambda rows: [
        pltpu.VMEM((NTGT, 256), bf16),
        pltpu.VMEM((TGT_TILES, 8, LANES), f32),
        pltpu.VMEM((rows, LANES), f32),
    ]
    g_tmp = [
        pltpu.VMEM((NSRC, 256), bf16),
        pltpu.VMEM((SRC_TILES, 8, LANES), f32),
        pltpu.VMEM((TGT_TILES, LANES), f32),
    ]
    w = log_weights.reshape(TGT_TILES, LANES)
    f_half, f_right, g_half, g_right, c, far, near, part = call(
        first_rows,
        (
            shape((NTGT, LANES), bf16),
            shape((256, NSRC), bf16),
            shape((NSRC, LANES), bf16),
            shape((256, NTGT), bf16),
            shape((TGT_TILES, LANES)),
            shape((TGT_TILES, LANES)),
            shape((SRC_TILES, LANES)),
            shape((n_tgt, 1, (SRC_TILES + 1) * LANES)),
        ),
        (generator, shift, targets, w),
        f_tmp(SRC_TILES + 8)
        + [
            pltpu.SMEM((DIM,), jnp.int32),
            pltpu.SMEM((DIM,), f32),
            pltpu.VMEM((DIM, NTGT), f32),
            pltpu.VMEM((TGT_TILES, LANES), f32),
            pltpu.SemaphoreType.DMA((4,)),
        ],
        space=pltpu.HBM,
    )
    got = exchanged(part, "tgt")
    norm, part = call(
        first_columns,
        (shape((8, LANES)), shape((n_src, TGT_TILES, LANES))),
        (got, g_half, g_right),
        g_tmp,
    )
    got = exchanged(part, "src")
    part = call(
        later_rows, shape((n_tgt, SRC_TILES, LANES)), (got, f_half, f_right, c), f_tmp(SRC_TILES)
    )
    got = exchanged(part, "tgt")
    every, part = call(
        later_columns,
        (shape((SRC_TILES, LANES)), shape((n_src, TGT_TILES, LANES))),
        (got, g_half, g_right, norm),
        g_tmp,
    )
    got = exchanged(part, "src")
    f, g = call(
        last_columns,
        (shape((SRC_TILES, LANES)), shape((TGT_TILES, LANES))),
        (got, far, every, near),
    )
    return f.reshape(NSRC), g.reshape(NTGT)


def solution(mesh):
    in_specs = (P(), P(), P(None, "tgt"), P("tgt"))
    out_specs = (P("src"), P("tgt"))
    return jax.shard_map(local, mesh=mesh, in_specs=in_specs, out_specs=out_specs, check_vma=False)
```

```python
import math
import jax
import jax.numpy as jnp
from jax import lax
from jax.experimental import pallas as pl
from jax.experimental.pallas import tpu as pltpu
from jax.sharding import PartitionSpec as P

DIM = 64
NSRC = 2048
NTGT = 1024
LANES = 128
SRC_TILES = NSRC // LANES
TGT_TILES = NTGT // LANES
FIRST_ROWS = SRC_TILES + 1
BLUR = 0.1
LOG2E = 1.4426950408889634
KAPPA = LOG2E / BLUR
UNKAPPA = 1.0 / KAPPA
WIDTH = 256
ROWS = 64
GRANT = 16 * 2**20
f32 = jnp.float32
bf16 = jnp.bfloat16

SINE = (6.28318530707259, -41.34170211699658, 81.6052262062997, -76.7042813207251, 42.00980570831026, -14.394135222236105)


def split(x):
    hi = x.astype(bf16)
    lo = (x - hi.astype(f32)).astype(bf16)
    return hi, lo


def pieces(x):
    first = x.astype(bf16).astype(f32)
    rest = x - first
    second = rest.astype(bf16).astype(f32)
    return first, second, rest - second


def column_of(values, kind):
    sub = lax.broadcasted_iota(jnp.int32, (8, LANES), 0)
    groups = []
    for g in range(DIM // 8):
        v = jnp.full((8, LANES), values[8 * g], kind)
        for s in range(1, 8):
            v = jnp.where(sub == s, values[8 * g + s], v)
        groups.append(v)
    return jnp.concatenate(groups, 0)


def sine_turns(u):
    r = u - jnp.floor(u + 0.5)
    a = jnp.abs(r)
    b = jnp.minimum(a, 0.5 - a)
    z = b * b
    p = jnp.full_like(z, SINE[-1])
    for c in SINE[-2::-1]:
        p = p * z + c
    v = b * p
    return jnp.where(r < 0, -v, v)


def place_terms(a_ref, d_ref, rows, tiles):
    d_ref[...] = jnp.zeros_like(d_ref)
    for k, piece in enumerate(pieces(rows)):
        d_ref[:, k, :] = piece
    for t in range(tiles):
        a_ref[LANES * t : LANES * (t + 1), LANES : LANES + 8] = d_ref[t].T.astype(bf16)


def fill_left(a_ref, half):
    lane = lax.broadcasted_iota(jnp.int32, half.shape, 1)
    a_ref[:, :LANES] = half
    a_ref[:, LANES:] = jnp.where(lane < 64, jnp.zeros_like(half), half)


def log_sums(a_ref, b_ref, out):
    for n in range(b_ref.shape[1] // WIDTH):
        s = jnp.dot(a_ref[...], b_ref[:, WIDTH * n : WIDTH * (n + 1)], preferred_element_type=f32)
        found = [([], []) for _ in range(WIDTH // LANES)]
        for m in range(0, s.shape[0], ROWS):
            for k, (tops, sums) in enumerate(found):
                block = s[m : m + ROWS, LANES * k : LANES * (k + 1)].reshape(ROWS // 8, 8, LANES)
                top = jnp.max(block, 0)
                tops.append(top)
                sums.append(jnp.sum(jnp.exp2(block - top[None]), 0))
        for k, (tops, sums) in enumerate(found):
            tops, sums = jnp.concatenate(tops, 0), jnp.concatenate(sums, 0)
            top = jnp.max(tops, 0, keepdims=True)
            r = n * (WIDTH // LANES) + k
            out[r : r + 1, :] = top + jnp.log2(jnp.sum(sums * jnp.exp2(tops - top), 0, keepdims=True))


def merged(parts):
    top = jnp.max(parts, 0)
    return top + jnp.log2(jnp.sum(jnp.exp2(parts - top[None]), 0))


def ones_rows():
    row = lax.broadcasted_iota(jnp.int32, (64, LANES), 0)
    return jnp.where(row < 3, 1.0, 0.0).astype(bf16)


def first_rows(
    gen_hbm, shift_hbm, t_hbm, w_hbm,
    half_ref, b_ref, g_half_ref, g_b_ref, c_ref, far_ref, near_ref, out_ref,
    a_ref, d_ref, l_ref, gen, shift, t_ref, w_ref, sems,
):
    moves = [
        pltpu.make_async_copy(src, dst, sems.at[k])
        for k, (src, dst) in enumerate(
            ((gen_hbm, gen), (shift_hbm, shift), (t_hbm, t_ref), (w_hbm, w_ref))
        )
    ]
    for move in moves:
        move.start()
    ones = ones_rows()
    offset = lax.axis_index("src") * NSRC
    modulus = NSRC * lax.axis_size("src")
    moves[0].wait()
    moves[1].wait()
    g = column_of(gen, jnp.int32)
    sh = column_of(shift, f32)
    lane = lax.broadcasted_iota(jnp.int32, (DIM, LANES), 1)
    turns = (((offset + lane) * g) & (modulus - 1)).astype(f32) * (1.0 / modulus) + sh
    step = ((LANES * g) & (modulus - 1)).astype(f32) * (1.0 / modulus)
    scaled, other = KAPPA * sine_turns(turns), KAPPA * sine_turns(turns + 0.25)
    step_sin, step_cos = sine_turns(step), sine_turns(step + 0.25)
    for t in range(SRC_TILES):
        cols = slice(LANES * t, LANES * (t + 1))
        near_ref[t : t + 1, :] = (0.5 * UNKAPPA**2) * jnp.sum(scaled * scaled, 0, keepdims=True)
        hi = scaled.astype(bf16).astype(f32)
        lo = scaled - hi
        b_ref[0:64, cols] = hi.astype(bf16)
        b_ref[64:128, cols] = hi.astype(bf16)
        b_ref[128:192, cols] = ones
        b_ref[192:256, cols] = lo.astype(bf16)
        g_half_ref[cols, :] = jnp.concatenate([lo, hi], 0).T.astype(bf16)
        scaled, other = scaled * step_cos + other * step_sin, other * step_cos - scaled * step_sin
    moves[2].wait()
    moves[3].wait()
    w = w_ref[...] * LOG2E
    c_ref[...] = w
    for t in range(TGT_TILES):
        rows = slice(LANES * t, LANES * (t + 1))
        y = t_ref[:, rows]
        far_ref[t : t + 1, :] = 0.5 * jnp.sum(y * y, 0, keepdims=True)
        hi = y.astype(bf16).astype(f32)
        half_ref[rows, :] = jnp.concatenate([y - hi, hi], 0).T.astype(bf16)
        g_b_ref[0:64, rows] = hi.astype(bf16)
        g_b_ref[64:128, rows] = hi.astype(bf16)
        g_b_ref[128:192, rows] = ones
        g_b_ref[192:256, rows] = (y - hi).astype(bf16)
    fill_left(a_ref, half_ref[...])
    place_terms(a_ref, d_ref, w - KAPPA * far_ref[...], TGT_TILES)
    top = jnp.max(w, keepdims=True)
    total = top + jnp.log2(jnp.sum(jnp.exp2(w - top), keepdims=True))
    log_sums(a_ref, b_ref, l_ref)
    l_ref[SRC_TILES:, :] = jnp.broadcast_to(total, (8, LANES))
    for d in range(0, out_ref.shape[0], FIRST_ROWS):
        out_ref[d : d + FIRST_ROWS, :] = l_ref[:FIRST_ROWS, :]


def first_columns(parts_ref, half_ref, b_ref, norm_ref, out_ref, a_ref, d_ref, l_ref):
    parts = [parts_ref[d : d + FIRST_ROWS, :] for d in range(0, parts_ref.shape[0], FIRST_ROWS)]
    top = parts[0]
    for part in parts[1:]:
        top = jnp.maximum(top, part)
    every = top + jnp.log2(sum(jnp.exp2(part - top) for part in parts))
    norm = every[SRC_TILES:, :]
    norm_ref[...] = jnp.broadcast_to(norm, norm_ref.shape)
    rows = (norm - every[:SRC_TILES, :]) - math.log2(NSRC * lax.axis_size("src"))
    fill_left(a_ref, half_ref[...])
    place_terms(a_ref, d_ref, rows, SRC_TILES)
    log_sums(a_ref, b_ref, l_ref)
    out_ref[...] = jnp.broadcast_to(l_ref[...][None], out_ref.shape)


def later_rows(parts_ref, half_ref, b_ref, c_ref, out_ref, a_ref, d_ref, l_ref):
    rows = c_ref[...] - merged(parts_ref[...])
    fill_left(a_ref, half_ref[...])
    place_terms(a_ref, d_ref, rows, TGT_TILES)
    log_sums(a_ref, b_ref, l_ref)
    out_ref[...] = jnp.broadcast_to(l_ref[...][None], out_ref.shape)


def later_columns(parts_ref, half_ref, b_ref, norm_ref, every_ref, out_ref, a_ref, d_ref, l_ref):
    every = merged(parts_ref[...]) - norm_ref[0:1, :]
    every_ref[...] = every
    fill_left(a_ref, half_ref[...])
    place_terms(a_ref, d_ref, -math.log2(NSRC * lax.axis_size("src")) - every, SRC_TILES)
    log_sums(a_ref, b_ref, l_ref)
    out_ref[...] = jnp.broadcast_to(l_ref[...][None], out_ref.shape)


def last_columns(parts_ref, far_ref, every_ref, near_ref, f_ref, g_ref):
    f_ref[...] = near_ref[...] - UNKAPPA * every_ref[...]
    g_ref[...] = far_ref[...] - UNKAPPA * merged(parts_ref[...])


def shape(dims, kind=f32):
    return jax.ShapeDtypeStruct(dims, kind)


def call(body, outs, inputs, scratch=(), space=pltpu.VMEM):
    if space is pltpu.HBM:
        inputs = [pltpu.with_memory_space_constraint(x, space) for x in inputs]
    return pl.pallas_call(
        body,
        out_shape=outs,
        in_specs=[pl.BlockSpec(memory_space=space)] * len(inputs),
        out_specs=jax.tree.map(lambda _: pl.BlockSpec(memory_space=pltpu.VMEM), outs),
        scratch_shapes=scratch,
        name=body.__name__,
        compiler_params=pltpu.CompilerParams(vmem_limit_bytes=GRANT),
    )(*inputs)


def exchanged(x, axis):
    return lax.all_to_all(x, axis, split_axis=0, concat_axis=0, tiled=True)


def local(generator, shift, targets, log_weights):
    n_src, n_tgt = lax.axis_size("src"), lax.axis_size("tgt")
    f_tmp = lambda rows: [
        pltpu.VMEM((NTGT, 256), bf16),
        pltpu.VMEM((TGT_TILES, 8, LANES), f32),
        pltpu.VMEM((rows, LANES), f32),
    ]
    g_tmp = [
        pltpu.VMEM((NSRC, 256), bf16),
        pltpu.VMEM((SRC_TILES, 8, LANES), f32),
        pltpu.VMEM((TGT_TILES, LANES), f32),
    ]
    w = log_weights.reshape(TGT_TILES, LANES)
    f_half, f_right, g_half, g_right, c, far, near, part = call(
        first_rows,
        (
            shape((NTGT, LANES), bf16),
            shape((256, NSRC), bf16),
            shape((NSRC, LANES), bf16),
            shape((256, NTGT), bf16),
            shape((TGT_TILES, LANES)),
            shape((TGT_TILES, LANES)),
            shape((SRC_TILES, LANES)),
            shape((n_tgt * FIRST_ROWS, LANES)),
        ),
        (generator, shift, targets, w),
        f_tmp(SRC_TILES + 8)
        + [
            pltpu.SMEM((DIM,), jnp.int32),
            pltpu.SMEM((DIM,), f32),
            pltpu.VMEM((DIM, NTGT), f32),
            pltpu.VMEM((TGT_TILES, LANES), f32),
            pltpu.SemaphoreType.DMA((4,)),
        ],
        space=pltpu.HBM,
    )
    part = part.reshape(n_tgt, 1, FIRST_ROWS * LANES)
    got = exchanged(part, "tgt").reshape(n_tgt * FIRST_ROWS, LANES)
    norm, part = call(
        first_columns,
        (shape((8, LANES)), shape((n_src, TGT_TILES, LANES))),
        (got, g_half, g_right),
        g_tmp,
    )
    got = exchanged(part, "src")
    part = call(
        later_rows, shape((n_tgt, SRC_TILES, LANES)), (got, f_half, f_right, c), f_tmp(SRC_TILES)
    )
    got = exchanged(part, "tgt")
    every, part = call(
        later_columns,
        (shape((SRC_TILES, LANES)), shape((n_src, TGT_TILES, LANES))),
        (got, g_half, g_right, norm),
        g_tmp,
    )
    got = exchanged(part, "src")
    f, g = call(
        last_columns,
        (shape((SRC_TILES, LANES)), shape((TGT_TILES, LANES))),
        (got, far, every, near),
    )
    return f.reshape(NSRC), g.reshape(NTGT)


def solution(mesh):
    in_specs = (P(), P(), P(None, "tgt"), P("tgt"))
    out_specs = (P("src"), P("tgt"))
    return jax.shard_map(local, mesh=mesh, in_specs=in_specs, out_specs=out_specs, check_vma=False)
```

```python
import math
import jax
import jax.numpy as jnp
from jax import lax
from jax.experimental import pallas as pl
from jax.experimental.pallas import tpu as pltpu
from jax.sharding import PartitionSpec as P

DIM = 64
NSRC = 2048
NTGT = 1024
LANES = 128
SRC_TILES = NSRC // LANES
TGT_TILES = NTGT // LANES
FIRST_ROWS = SRC_TILES + 1
BLUR = 0.1
LOG2E = 1.4426950408889634
KAPPA = LOG2E / BLUR
UNKAPPA = 1.0 / KAPPA
WIDTH = 256
ROWS = 64
GRANT = 16 * 2**20
FIRST = {"src": 4, "tgt": 21}
f32 = jnp.float32
bf16 = jnp.bfloat16

SINE = (6.28318530707259, -41.34170211699658, 81.6052262062997, -76.7042813207251, 42.00980570831026, -14.394135222236105)


def split(x):
    hi = x.astype(bf16)
    lo = (x - hi.astype(f32)).astype(bf16)
    return hi, lo


def pieces(x):
    first = x.astype(bf16).astype(f32)
    rest = x - first
    second = rest.astype(bf16).astype(f32)
    return first, second, rest - second


def column_of(values, kind):
    sub = lax.broadcasted_iota(jnp.int32, (8, LANES), 0)
    groups = []
    for g in range(DIM // 8):
        v = jnp.full((8, LANES), values[8 * g], kind)
        for s in range(1, 8):
            v = jnp.where(sub == s, values[8 * g + s], v)
        groups.append(v)
    return jnp.concatenate(groups, 0)


def sine_turns(u):
    r = u - jnp.floor(u + 0.5)
    a = jnp.abs(r)
    b = jnp.minimum(a, 0.5 - a)
    z = b * b
    p = jnp.full_like(z, SINE[-1])
    for c in SINE[-2::-1]:
        p = p * z + c
    v = b * p
    return jnp.where(r < 0, -v, v)


def place_terms(a_ref, d_ref, rows, tiles):
    d_ref[...] = jnp.zeros_like(d_ref)
    for k, piece in enumerate(pieces(rows)):
        d_ref[:, k, :] = piece
    for t in range(tiles):
        a_ref[LANES * t : LANES * (t + 1), 0:8] = d_ref[t].T.astype(bf16)


def fill_left(a_ref, half):
    lane = lax.broadcasted_iota(jnp.int32, half.shape, 1)
    a_ref[...] = jnp.where(lane < 64, jnp.zeros_like(half), half)


def log_sums(half_ref, a_ref, b_ref, out):
    for n in range(b_ref.shape[1] // WIDTH):
        a = jnp.concatenate([half_ref[...], a_ref[...]], 1)
        s = jnp.dot(a, b_ref[:, WIDTH * n : WIDTH * (n + 1)], preferred_element_type=f32)
        found = [([], []) for _ in range(WIDTH // LANES)]
        for m in range(0, s.shape[0], ROWS):
            for k, (tops, sums) in enumerate(found):
                block = s[m : m + ROWS, LANES * k : LANES * (k + 1)].reshape(ROWS // 8, 8, LANES)
                top = jnp.max(block, 0)
                tops.append(top)
                sums.append(jnp.sum(jnp.exp2(block - top[None]), 0))
        for k, (tops, sums) in enumerate(found):
            tops, sums = jnp.concatenate(tops, 0), jnp.concatenate(sums, 0)
            top = jnp.max(tops, 0, keepdims=True)
            r = n * (WIDTH // LANES) + k
            out[r : r + 1, :] = top + jnp.log2(jnp.sum(sums * jnp.exp2(tops - top), 0, keepdims=True))


def merged(parts):
    top = jnp.max(parts, 0)
    return top + jnp.log2(jnp.sum(jnp.exp2(parts - top[None]), 0))


def ones_rows():
    row = lax.broadcasted_iota(jnp.int32, (64, LANES), 0)
    return jnp.where(row < 3, 1.0, 0.0).astype(bf16)


def first_rows(
    gen_hbm, shift_hbm, t_hbm, w_hbm,
    half_ref, b_ref, g_half_ref, g_b_ref, c_ref, far_ref, near_ref, out_ref,
    a_ref, d_ref, l_ref, gen, shift, t_ref, w_ref, sems,
):
    moves = [
        pltpu.make_async_copy(src, dst, sems.at[k])
        for k, (src, dst) in enumerate(
            ((gen_hbm, gen), (shift_hbm, shift), (t_hbm, t_ref), (w_hbm, w_ref))
        )
    ]
    for move in moves:
        move.start()
    ones = ones_rows()
    offset = lax.axis_index("src") * NSRC
    modulus = NSRC * lax.axis_size("src")
    moves[0].wait()
    moves[1].wait()
    g = column_of(gen, jnp.int32)
    sh = column_of(shift, f32)
    lane = lax.broadcasted_iota(jnp.int32, (DIM, LANES), 1)
    turns = (((offset + lane) * g) & (modulus - 1)).astype(f32) * (1.0 / modulus) + sh
    step = ((LANES * g) & (modulus - 1)).astype(f32) * (1.0 / modulus)
    scaled, other = KAPPA * sine_turns(turns), KAPPA * sine_turns(turns + 0.25)
    step_sin, step_cos = sine_turns(step), sine_turns(step + 0.25)
    for t in range(SRC_TILES):
        cols = slice(LANES * t, LANES * (t + 1))
        near_ref[t : t + 1, :] = (0.5 * UNKAPPA**2) * jnp.sum(scaled * scaled, 0, keepdims=True)
        hi = scaled.astype(bf16).astype(f32)
        lo = scaled - hi
        b_ref[0:64, cols] = hi.astype(bf16)
        b_ref[64:128, cols] = hi.astype(bf16)
        b_ref[128:192, cols] = ones
        b_ref[192:256, cols] = lo.astype(bf16)
        g_half_ref[cols, :] = jnp.concatenate([lo, hi], 0).T.astype(bf16)
        scaled, other = scaled * step_cos + other * step_sin, other * step_cos - scaled * step_sin
    moves[2].wait()
    moves[3].wait()
    w = w_ref[...] * LOG2E
    c_ref[...] = w
    for t in range(TGT_TILES):
        rows = slice(LANES * t, LANES * (t + 1))
        y = t_ref[:, rows]
        far_ref[t : t + 1, :] = 0.5 * jnp.sum(y * y, 0, keepdims=True)
        hi = y.astype(bf16).astype(f32)
        half_ref[rows, :] = jnp.concatenate([y - hi, hi], 0).T.astype(bf16)
        g_b_ref[0:64, rows] = hi.astype(bf16)
        g_b_ref[64:128, rows] = hi.astype(bf16)
        g_b_ref[128:192, rows] = ones
        g_b_ref[192:256, rows] = (y - hi).astype(bf16)
    fill_left(a_ref, half_ref[...])
    place_terms(a_ref, d_ref, w - KAPPA * far_ref[...], TGT_TILES)
    top = jnp.max(w, keepdims=True)
    total = top + jnp.log2(jnp.sum(jnp.exp2(w - top), keepdims=True))
    log_sums(half_ref, a_ref, b_ref, l_ref)
    l_ref[SRC_TILES:, :] = jnp.broadcast_to(total, (8, LANES))
    for d in range(0, out_ref.shape[0], FIRST_ROWS):
        out_ref[d : d + FIRST_ROWS, :] = l_ref[:FIRST_ROWS, :]


def first_columns(parts_ref, half_ref, b_ref, norm_ref, out_ref, a_ref, d_ref, l_ref):
    parts = [parts_ref[d : d + FIRST_ROWS, :] for d in range(0, parts_ref.shape[0], FIRST_ROWS)]
    top = parts[0]
    for part in parts[1:]:
        top = jnp.maximum(top, part)
    every = top + jnp.log2(sum(jnp.exp2(part - top) for part in parts))
    norm = every[SRC_TILES:, :]
    norm_ref[...] = jnp.broadcast_to(norm, norm_ref.shape)
    rows = (norm - every[:SRC_TILES, :]) - math.log2(NSRC * lax.axis_size("src"))
    fill_left(a_ref, half_ref[...])
    place_terms(a_ref, d_ref, rows, SRC_TILES)
    log_sums(half_ref, a_ref, b_ref, l_ref)
    out_ref[...] = jnp.broadcast_to(l_ref[...][None], out_ref.shape)


def later_rows(parts_ref, half_ref, b_ref, c_ref, out_ref, a_ref, d_ref, l_ref):
    rows = c_ref[...] - merged(parts_ref[...])
    fill_left(a_ref, half_ref[...])
    place_terms(a_ref, d_ref, rows, TGT_TILES)
    log_sums(half_ref, a_ref, b_ref, l_ref)
    out_ref[...] = jnp.broadcast_to(l_ref[...][None], out_ref.shape)


def later_columns(parts_ref, half_ref, b_ref, norm_ref, every_ref, out_ref, a_ref, d_ref, l_ref):
    every = merged(parts_ref[...]) - norm_ref[0:1, :]
    every_ref[...] = every
    fill_left(a_ref, half_ref[...])
    place_terms(a_ref, d_ref, -math.log2(NSRC * lax.axis_size("src")) - every, SRC_TILES)
    log_sums(half_ref, a_ref, b_ref, l_ref)
    out_ref[...] = jnp.broadcast_to(l_ref[...][None], out_ref.shape)


def last_columns(parts_ref, far_ref, every_ref, near_ref, f_ref, g_ref):
    f_ref[...] = near_ref[...] - UNKAPPA * every_ref[...]
    g_ref[...] = far_ref[...] - UNKAPPA * merged(parts_ref[...])


def shape(dims, kind=f32):
    return jax.ShapeDtypeStruct(dims, kind)


def call(body, outs, inputs, scratch=(), space=pltpu.VMEM):
    if space is pltpu.HBM:
        inputs = [pltpu.with_memory_space_constraint(x, space) for x in inputs]
    return pl.pallas_call(
        body,
        out_shape=outs,
        in_specs=[pl.BlockSpec(memory_space=space)] * len(inputs),
        out_specs=jax.tree.map(lambda _: pl.BlockSpec(memory_space=pltpu.VMEM), outs),
        scratch_shapes=scratch,
        name=body.__name__,
        compiler_params=pltpu.CompilerParams(vmem_limit_bytes=GRANT),
    )(*inputs)


def exchanged(x, axis):
    n, first = lax.axis_size(axis), FIRST[axis]
    order = [(first + k) % n for k in range(n)]
    return lax.all_to_all(
        x, axis, split_axis=0, concat_axis=0, axis_index_groups=[order], tiled=True
    )


def local(generator, shift, targets, log_weights):
    n_src, n_tgt = lax.axis_size("src"), lax.axis_size("tgt")
    f_tmp = lambda rows: [
        pltpu.VMEM((NTGT, LANES), bf16),
        pltpu.VMEM((TGT_TILES, 8, LANES), f32),
        pltpu.VMEM((rows, LANES), f32),
    ]
    g_tmp = [
        pltpu.VMEM((NSRC, LANES), bf16),
        pltpu.VMEM((SRC_TILES, 8, LANES), f32),
        pltpu.VMEM((TGT_TILES, LANES), f32),
    ]
    w = log_weights.reshape(TGT_TILES, LANES)
    f_half, f_right, g_half, g_right, c, far, near, part = call(
        first_rows,
        (
            shape((NTGT, LANES), bf16),
            shape((256, NSRC), bf16),
            shape((NSRC, LANES), bf16),
            shape((256, NTGT), bf16),
            shape((TGT_TILES, LANES)),
            shape((TGT_TILES, LANES)),
            shape((SRC_TILES, LANES)),
            shape((n_tgt * FIRST_ROWS, LANES)),
        ),
        (generator, shift, targets, w),
        f_tmp(SRC_TILES + 8)
        + [
            pltpu.SMEM((DIM,), jnp.int32),
            pltpu.SMEM((DIM,), f32),
            pltpu.VMEM((DIM, NTGT), f32),
            pltpu.VMEM((TGT_TILES, LANES), f32),
            pltpu.SemaphoreType.DMA((4,)),
        ],
        space=pltpu.HBM,
    )
    part = part.reshape(n_tgt, 1, FIRST_ROWS * LANES)
    got = exchanged(part, "tgt").reshape(n_tgt * FIRST_ROWS, LANES)
    norm, part = call(
        first_columns,
        (shape((8, LANES)), shape((n_src, TGT_TILES, LANES))),
        (got, g_half, g_right),
        g_tmp,
    )
    got = exchanged(part, "src")
    part = call(
        later_rows, shape((n_tgt, SRC_TILES, LANES)), (got, f_half, f_right, c), f_tmp(SRC_TILES)
    )
    got = exchanged(part, "tgt")
    every, part = call(
        later_columns,
        (shape((SRC_TILES, LANES)), shape((n_src, TGT_TILES, LANES))),
        (got, g_half, g_right, norm),
        g_tmp,
    )
    got = exchanged(part, "src")
    f, g = call(
        last_columns,
        (shape((SRC_TILES, LANES)), shape((TGT_TILES, LANES))),
        (got, far, every, near),
    )
    return f.reshape(NSRC), g.reshape(NTGT)


def solution(mesh):
    in_specs = (P(), P(), P(None, "tgt"), P("tgt"))
    out_specs = (P("src"), P("tgt"))
    return jax.shard_map(local, mesh=mesh, in_specs=in_specs, out_specs=out_specs, check_vma=False)
```

```python
import math
import jax
import jax.numpy as jnp
from jax import lax
from jax.experimental import pallas as pl
from jax.experimental.pallas import tpu as pltpu
from jax.sharding import PartitionSpec as P

DIM = 64
NSRC = 2048
NTGT = 1024
LANES = 128
SRC_TILES = NSRC // LANES
TGT_TILES = NTGT // LANES
FIRST_ROWS = SRC_TILES + 1
BLUR = 0.1
LOG2E = 1.4426950408889634
KAPPA = LOG2E / BLUR
UNKAPPA = 1.0 / KAPPA
WIDTH = 256
ROWS = 64
EARLY = 4
GRANT = 16 * 2**20
ORDER = {"src": [4, 0, 1, 7, 2, 6, 3, 5], "tgt": [(21 + k) % 32 for k in range(32)]}
f32 = jnp.float32
bf16 = jnp.bfloat16

SINE = (6.28318530707259, -41.34170211699658, 81.6052262062997, -76.7042813207251, 42.00980570831026, -14.394135222236105)


def split(x):
    hi = x.astype(bf16)
    lo = (x - hi.astype(f32)).astype(bf16)
    return hi, lo


def pieces(x):
    first = x.astype(bf16).astype(f32)
    rest = x - first
    second = rest.astype(bf16).astype(f32)
    return first, second, rest - second


def column_of(values, kind):
    sub = lax.broadcasted_iota(jnp.int32, (8, LANES), 0)
    groups = []
    for g in range(DIM // 8):
        v = jnp.full((8, LANES), values[8 * g], kind)
        for s in range(1, 8):
            v = jnp.where(sub == s, values[8 * g + s], v)
        groups.append(v)
    return jnp.concatenate(groups, 0)


def sine_turns(u):
    r = u - jnp.floor(u + 0.5)
    a = jnp.abs(r)
    b = jnp.minimum(a, 0.5 - a)
    z = b * b
    p = jnp.full_like(z, SINE[-1])
    for c in SINE[-2::-1]:
        p = p * z + c
    v = b * p
    return jnp.where(r < 0, -v, v)


def place_terms(a_ref, d_ref, rows, tiles):
    d_ref[...] = jnp.zeros_like(d_ref)
    for k, piece in enumerate(pieces(rows)):
        d_ref[:, k, :] = piece
    for t in range(tiles):
        a_ref[LANES * t : LANES * (t + 1), 0:8] = d_ref[t].T.astype(bf16)


def fill_left(a_ref, half):
    lane = lax.broadcasted_iota(jnp.int32, half.shape, 1)
    a_ref[...] = jnp.where(lane < 64, jnp.zeros_like(half), half)


def log_sums(half_ref, a_ref, b_ref, out):
    for n in range(b_ref.shape[1] // WIDTH):
        a = jnp.concatenate([half_ref[...], a_ref[...]], 1)
        s = jnp.dot(a, b_ref[:, WIDTH * n : WIDTH * (n + 1)], preferred_element_type=f32)
        found = [([], []) for _ in range(WIDTH // LANES)]
        for m in range(0, s.shape[0], ROWS):
            for k, (tops, sums) in enumerate(found):
                block = s[m : m + ROWS, LANES * k : LANES * (k + 1)].reshape(ROWS // 8, 8, LANES)
                top = jnp.max(block, 0)
                tops.append(top)
                sums.append(jnp.sum(jnp.exp2(block - top[None]), 0))
        for k, (tops, sums) in enumerate(found):
            tops, sums = jnp.concatenate(tops, 0), jnp.concatenate(sums, 0)
            top = jnp.max(tops, 0, keepdims=True)
            r = n * (WIDTH // LANES) + k
            out[r : r + 1, :] = top + jnp.log2(jnp.sum(sums * jnp.exp2(tops - top), 0, keepdims=True))


def merged(parts):
    top = jnp.max(parts, 0)
    return top + jnp.log2(jnp.sum(jnp.exp2(parts - top[None]), 0))


def ones_rows():
    row = lax.broadcasted_iota(jnp.int32, (64, LANES), 0)
    return jnp.where(row < 3, 1.0, 0.0).astype(bf16)


def first_rows(
    gen_hbm, shift_hbm, t_hbm, w_hbm,
    half_ref, b_ref, g_half_ref, g_b_ref, c_ref, far_ref, near_ref, out_ref,
    a_ref, d_ref, l_ref, gen, shift, t_ref, w_ref, sems,
):
    moves = [
        pltpu.make_async_copy(src, dst, sems.at[k])
        for k, (src, dst) in enumerate(
            ((gen_hbm, gen), (shift_hbm, shift), (t_hbm, t_ref), (w_hbm, w_ref))
        )
    ]
    for move in moves:
        move.start()
    ones = ones_rows()
    for t in range(SRC_TILES):
        b_ref[128:192, LANES * t : LANES * (t + 1)] = ones
    for t in range(TGT_TILES):
        g_b_ref[128:192, LANES * t : LANES * (t + 1)] = ones
    offset = lax.axis_index("src") * NSRC
    modulus = NSRC * lax.axis_size("src")
    moves[0].wait()
    moves[1].wait()
    g = column_of(gen, jnp.int32)
    sh = column_of(shift, f32)
    lane = lax.broadcasted_iota(jnp.int32, (DIM, LANES), 1)
    turns = (((offset + lane) * g) & (modulus - 1)).astype(f32) * (1.0 / modulus) + sh
    step = ((LANES * g) & (modulus - 1)).astype(f32) * (1.0 / modulus)
    scaled, other = KAPPA * sine_turns(turns), KAPPA * sine_turns(turns + 0.25)
    step_sin, step_cos = sine_turns(step), sine_turns(step + 0.25)
    def put(t, scaled, other):
        cols = slice(LANES * t, LANES * (t + 1))
        near_ref[t : t + 1, :] = (0.5 * UNKAPPA**2) * jnp.sum(scaled * scaled, 0, keepdims=True)
        hi = scaled.astype(bf16).astype(f32)
        lo = scaled - hi
        b_ref[0:64, cols] = hi.astype(bf16)
        b_ref[64:128, cols] = hi.astype(bf16)
        b_ref[192:256, cols] = lo.astype(bf16)
        g_half_ref[cols, :] = jnp.concatenate([lo, hi], 0).T.astype(bf16)
        return scaled * step_cos + other * step_sin, other * step_cos - scaled * step_sin

    for t in range(EARLY):
        scaled, other = put(t, scaled, other)
    moves[2].wait()
    moves[3].wait()
    w = w_ref[...] * LOG2E
    c_ref[...] = w
    for t in range(TGT_TILES):
        rows = slice(LANES * t, LANES * (t + 1))
        y = t_ref[:, rows]
        far_ref[t : t + 1, :] = 0.5 * jnp.sum(y * y, 0, keepdims=True)
        hi = y.astype(bf16).astype(f32)
        half_ref[rows, :] = jnp.concatenate([y - hi, hi], 0).T.astype(bf16)
        g_b_ref[0:64, rows] = hi.astype(bf16)
        g_b_ref[64:128, rows] = hi.astype(bf16)
        g_b_ref[192:256, rows] = (y - hi).astype(bf16)
    fill_left(a_ref, half_ref[...])
    place_terms(a_ref, d_ref, w - KAPPA * far_ref[...], TGT_TILES)
    for t in range(EARLY, SRC_TILES):
        scaled, other = put(t, scaled, other)
    top = jnp.max(w, keepdims=True)
    total = top + jnp.log2(jnp.sum(jnp.exp2(w - top), keepdims=True))
    log_sums(half_ref, a_ref, b_ref, l_ref)
    l_ref[SRC_TILES:, :] = jnp.broadcast_to(total, (8, LANES))
    for d in range(0, out_ref.shape[0], FIRST_ROWS):
        out_ref[d : d + FIRST_ROWS, :] = l_ref[:FIRST_ROWS, :]


def first_columns(parts_ref, half_ref, b_ref, norm_ref, out_ref, a_ref, d_ref, l_ref):
    parts = [parts_ref[d : d + FIRST_ROWS, :] for d in range(0, parts_ref.shape[0], FIRST_ROWS)]
    top = parts[0]
    for part in parts[1:]:
        top = jnp.maximum(top, part)
    every = top + jnp.log2(sum(jnp.exp2(part - top) for part in parts))
    norm = every[SRC_TILES:, :]
    norm_ref[...] = jnp.broadcast_to(norm, norm_ref.shape)
    rows = (norm - every[:SRC_TILES, :]) - math.log2(NSRC * lax.axis_size("src"))
    fill_left(a_ref, half_ref[...])
    place_terms(a_ref, d_ref, rows, SRC_TILES)
    log_sums(half_ref, a_ref, b_ref, l_ref)
    out_ref[...] = jnp.broadcast_to(l_ref[...][None], out_ref.shape)


def later_rows(parts_ref, half_ref, b_ref, c_ref, out_ref, a_ref, d_ref, l_ref):
    rows = c_ref[...] - merged(parts_ref[...])
    fill_left(a_ref, half_ref[...])
    place_terms(a_ref, d_ref, rows, TGT_TILES)
    log_sums(half_ref, a_ref, b_ref, l_ref)
    out_ref[...] = jnp.broadcast_to(l_ref[...][None], out_ref.shape)


def later_columns(parts_ref, half_ref, b_ref, norm_ref, every_ref, out_ref, a_ref, d_ref, l_ref):
    every = merged(parts_ref[...]) - norm_ref[0:1, :]
    every_ref[...] = every
    fill_left(a_ref, half_ref[...])
    place_terms(a_ref, d_ref, -math.log2(NSRC * lax.axis_size("src")) - every, SRC_TILES)
    log_sums(half_ref, a_ref, b_ref, l_ref)
    out_ref[...] = jnp.broadcast_to(l_ref[...][None], out_ref.shape)


def last_columns(parts_ref, far_ref, every_ref, near_ref, f_ref, g_ref):
    f_ref[...] = near_ref[...] - UNKAPPA * every_ref[...]
    g_ref[...] = far_ref[...] - UNKAPPA * merged(parts_ref[...])


def shape(dims, kind=f32):
    return jax.ShapeDtypeStruct(dims, kind)


def call(body, outs, inputs, scratch=(), space=pltpu.VMEM):
    if space is pltpu.HBM:
        inputs = [pltpu.with_memory_space_constraint(x, space) for x in inputs]
    return pl.pallas_call(
        body,
        out_shape=outs,
        in_specs=[pl.BlockSpec(memory_space=space)] * len(inputs),
        out_specs=jax.tree.map(lambda _: pl.BlockSpec(memory_space=pltpu.VMEM), outs),
        scratch_shapes=scratch,
        name=body.__name__,
        compiler_params=pltpu.CompilerParams(vmem_limit_bytes=GRANT),
    )(*inputs)


def exchanged(x, axis):
    return lax.all_to_all(
        x, axis, split_axis=0, concat_axis=0, axis_index_groups=[ORDER[axis]], tiled=True
    )


def local(generator, shift, targets, log_weights):
    n_src, n_tgt = lax.axis_size("src"), lax.axis_size("tgt")
    f_tmp = lambda rows: [
        pltpu.VMEM((NTGT, LANES), bf16),
        pltpu.VMEM((TGT_TILES, 8, LANES), f32),
        pltpu.VMEM((rows, LANES), f32),
    ]
    g_tmp = [
        pltpu.VMEM((NSRC, LANES), bf16),
        pltpu.VMEM((SRC_TILES, 8, LANES), f32),
        pltpu.VMEM((TGT_TILES, LANES), f32),
    ]
    w = log_weights.reshape(TGT_TILES, LANES)
    f_half, f_right, g_half, g_right, c, far, near, part = call(
        first_rows,
        (
            shape((NTGT, LANES), bf16),
            shape((256, NSRC), bf16),
            shape((NSRC, LANES), bf16),
            shape((256, NTGT), bf16),
            shape((TGT_TILES, LANES)),
            shape((TGT_TILES, LANES)),
            shape((SRC_TILES, LANES)),
            shape((n_tgt * FIRST_ROWS, LANES)),
        ),
        (generator, shift, targets, w),
        f_tmp(SRC_TILES + 8)
        + [
            pltpu.SMEM((DIM,), jnp.int32),
            pltpu.SMEM((DIM,), f32),
            pltpu.VMEM((DIM, NTGT), f32),
            pltpu.VMEM((TGT_TILES, LANES), f32),
            pltpu.SemaphoreType.DMA((4,)),
        ],
        space=pltpu.HBM,
    )
    part = part.reshape(n_tgt, 1, FIRST_ROWS * LANES)
    got = exchanged(part, "tgt").reshape(n_tgt * FIRST_ROWS, LANES)
    norm, part = call(
        first_columns,
        (shape((8, LANES)), shape((n_src, TGT_TILES, LANES))),
        (got, g_half, g_right),
        g_tmp,
    )
    got = exchanged(part, "src")
    part = call(
        later_rows, shape((n_tgt, SRC_TILES, LANES)), (got, f_half, f_right, c), f_tmp(SRC_TILES)
    )
    got = exchanged(part, "tgt")
    every, part = call(
        later_columns,
        (shape((SRC_TILES, LANES)), shape((n_src, TGT_TILES, LANES))),
        (got, g_half, g_right, norm),
        g_tmp,
    )
    got = exchanged(part, "src")
    f, g = call(
        last_columns,
        (shape((SRC_TILES, LANES)), shape((TGT_TILES, LANES))),
        (got, far, every, near),
    )
    return f.reshape(NSRC), g.reshape(NTGT)


def solution(mesh):
    in_specs = (P(), P(), P(None, "tgt"), P("tgt"))
    out_specs = (P("src"), P("tgt"))
    return jax.shard_map(local, mesh=mesh, in_specs=in_specs, out_specs=out_specs, check_vma=False)
```

```python
import math
import jax
import jax.numpy as jnp
from jax import lax
from jax.experimental import pallas as pl
from jax.experimental.pallas import tpu as pltpu
from jax.sharding import PartitionSpec as P

DIM = 64
NSRC = 2048
NTGT = 1024
LANES = 128
SRC_TILES = NSRC // LANES
TGT_TILES = NTGT // LANES
FIRST_ROWS = SRC_TILES + 1
BLUR = 0.1
LOG2E = 1.4426950408889634
KAPPA = LOG2E / BLUR
UNKAPPA = 1.0 / KAPPA
WIDTH = 256
ROWS = 64
SPLIT = 4
EARLY = 4
GRANT = 16 * 2**20
ORDER = {"src": [4, 0, 1, 7, 2, 6, 3, 5], "tgt": [(21 + k) % 32 for k in range(32)]}
f32 = jnp.float32
bf16 = jnp.bfloat16

SINE = (6.28318530707259, -41.34170211699658, 81.6052262062997, -76.7042813207251, 42.00980570831026, -14.394135222236105)


def split(x):
    hi = x.astype(bf16)
    lo = (x - hi.astype(f32)).astype(bf16)
    return hi, lo


def pieces(x):
    first = x.astype(bf16).astype(f32)
    rest = x - first
    second = rest.astype(bf16).astype(f32)
    return first, second, rest - second


def column_of(values, kind):
    sub = lax.broadcasted_iota(jnp.int32, (8, LANES), 0)
    groups = []
    for g in range(DIM // 8):
        v = jnp.full((8, LANES), values[8 * g], kind)
        for s in range(1, 8):
            v = jnp.where(sub == s, values[8 * g + s], v)
        groups.append(v)
    return jnp.concatenate(groups, 0)


def sine_turns(u):
    r = u - jnp.floor(u + 0.5)
    a = jnp.abs(r)
    b = jnp.minimum(a, 0.5 - a)
    z = b * b
    p = jnp.full_like(z, SINE[-1])
    for c in SINE[-2::-1]:
        p = p * z + c
    v = b * p
    return jnp.where(r < 0, -v, v)


def place_terms(a_ref, d_ref, rows, tiles):
    d_ref[...] = jnp.zeros_like(d_ref)
    for k, piece in enumerate(pieces(rows)):
        d_ref[:, k, :] = piece
    for t in range(tiles):
        a_ref[LANES * t : LANES * (t + 1), 0:8] = d_ref[t].T.astype(bf16)


def fill_left(a_ref, half):
    lane = lax.broadcasted_iota(jnp.int32, half.shape, 1)
    a_ref[...] = jnp.where(lane < 64, jnp.zeros_like(half), half)


def log_sums(half_ref, a_ref, b_ref, out):
    for n in range(b_ref.shape[1] // WIDTH):
        a = jnp.concatenate([half_ref[...], a_ref[...]], 1)
        s = jnp.dot(a, b_ref[:, WIDTH * n : WIDTH * (n + 1)], preferred_element_type=f32)
        found = [([], []) for _ in range(WIDTH // LANES)]
        for m in range(0, s.shape[0], ROWS):
            for k, (tops, sums) in enumerate(found):
                block = s[m : m + ROWS, LANES * k : LANES * (k + 1)].reshape(ROWS // 8, 8, LANES)
                top = jnp.max(block, 0)
                tops.append(top)
                sums.append(jnp.sum(jnp.exp2(block - top[None]), 0))
        for k, (tops, sums) in enumerate(found):
            tops, sums = jnp.concatenate(tops, 0), jnp.concatenate(sums, 0)
            top = jnp.max(tops, 0, keepdims=True)
            r = n * (WIDTH // LANES) + k
            out[r : r + 1, :] = top + jnp.log2(jnp.sum(sums * jnp.exp2(tops - top), 0, keepdims=True))


def merged(parts):
    top = jnp.max(parts, 0)
    return top + jnp.log2(jnp.sum(jnp.exp2(parts - top[None]), 0))


def ones_rows():
    row = lax.broadcasted_iota(jnp.int32, (64, LANES), 0)
    return jnp.where(row < 3, 1.0, 0.0).astype(bf16)


def first_rows(
    gen_hbm, shift_hbm, t_hbm, w_hbm,
    half_ref, b_ref, g_half_ref, g_b_ref, c_ref, far_ref, near_ref, out_ref,
    a_ref, d_ref, l_ref, gen, shift, t_ref, w_ref, sems,
):
    pairs = [(gen_hbm, gen), (shift_hbm, shift), (w_hbm, w_ref)]
    for k in range(0, DIM, DIM // SPLIT):
        rows = pl.ds(k, DIM // SPLIT)
        pairs.append((t_hbm.at[rows], t_ref.at[rows]))
    moves = [pltpu.make_async_copy(src, dst, sems.at[k]) for k, (src, dst) in enumerate(pairs)]
    for move in moves:
        move.start()
    ones = ones_rows()
    for t in range(SRC_TILES):
        b_ref[128:192, LANES * t : LANES * (t + 1)] = ones
    for t in range(TGT_TILES):
        g_b_ref[128:192, LANES * t : LANES * (t + 1)] = ones
    offset = lax.axis_index("src") * NSRC
    modulus = NSRC * lax.axis_size("src")
    moves[0].wait()
    moves[1].wait()
    g = column_of(gen, jnp.int32)
    sh = column_of(shift, f32)
    lane = lax.broadcasted_iota(jnp.int32, (DIM, LANES), 1)
    turns = (((offset + lane) * g) & (modulus - 1)).astype(f32) * (1.0 / modulus) + sh
    step = ((LANES * g) & (modulus - 1)).astype(f32) * (1.0 / modulus)
    scaled, other = KAPPA * sine_turns(turns), KAPPA * sine_turns(turns + 0.25)
    step_sin, step_cos = sine_turns(step), sine_turns(step + 0.25)
    def put(t, scaled, other):
        cols = slice(LANES * t, LANES * (t + 1))
        near_ref[t : t + 1, :] = (0.5 * UNKAPPA**2) * jnp.sum(scaled * scaled, 0, keepdims=True)
        hi = scaled.astype(bf16).astype(f32)
        lo = scaled - hi
        b_ref[0:64, cols] = hi.astype(bf16)
        b_ref[64:128, cols] = hi.astype(bf16)
        b_ref[192:256, cols] = lo.astype(bf16)
        g_half_ref[cols, :] = jnp.concatenate([lo, hi], 0).T.astype(bf16)
        return scaled * step_cos + other * step_sin, other * step_cos - scaled * step_sin

    for t in range(EARLY):
        scaled, other = put(t, scaled, other)
    for move in moves[2:]:
        move.wait()
    w = w_ref[...] * LOG2E
    c_ref[...] = w
    for t in range(TGT_TILES):
        rows = slice(LANES * t, LANES * (t + 1))
        y = t_ref[:, rows]
        far_ref[t : t + 1, :] = 0.5 * jnp.sum(y * y, 0, keepdims=True)
        hi = y.astype(bf16).astype(f32)
        half_ref[rows, :] = jnp.concatenate([y - hi, hi], 0).T.astype(bf16)
        g_b_ref[0:64, rows] = hi.astype(bf16)
        g_b_ref[64:128, rows] = hi.astype(bf16)
        g_b_ref[192:256, rows] = (y - hi).astype(bf16)
    fill_left(a_ref, half_ref[...])
    place_terms(a_ref, d_ref, w - KAPPA * far_ref[...], TGT_TILES)
    for t in range(EARLY, SRC_TILES):
        scaled, other = put(t, scaled, other)
    top = jnp.max(w, keepdims=True)
    total = top + jnp.log2(jnp.sum(jnp.exp2(w - top), keepdims=True))
    log_sums(half_ref, a_ref, b_ref, l_ref)
    l_ref[SRC_TILES:, :] = jnp.broadcast_to(total, (8, LANES))
    for d in range(0, out_ref.shape[0], FIRST_ROWS):
        out_ref[d : d + FIRST_ROWS, :] = l_ref[:FIRST_ROWS, :]


def first_columns(parts_ref, half_ref, b_ref, norm_ref, out_ref, a_ref, d_ref, l_ref):
    parts = [parts_ref[d : d + FIRST_ROWS, :] for d in range(0, parts_ref.shape[0], FIRST_ROWS)]
    top = parts[0]
    for part in parts[1:]:
        top = jnp.maximum(top, part)
    every = top + jnp.log2(sum(jnp.exp2(part - top) for part in parts))
    norm = every[SRC_TILES:, :]
    norm_ref[...] = jnp.broadcast_to(norm, norm_ref.shape)
    rows = (norm - every[:SRC_TILES, :]) - math.log2(NSRC * lax.axis_size("src"))
    fill_left(a_ref, half_ref[...])
    place_terms(a_ref, d_ref, rows, SRC_TILES)
    log_sums(half_ref, a_ref, b_ref, l_ref)
    out_ref[...] = jnp.broadcast_to(l_ref[...][None], out_ref.shape)


def later_rows(parts_ref, half_ref, b_ref, c_ref, out_ref, a_ref, d_ref, l_ref):
    rows = c_ref[...] - merged(parts_ref[...])
    fill_left(a_ref, half_ref[...])
    place_terms(a_ref, d_ref, rows, TGT_TILES)
    log_sums(half_ref, a_ref, b_ref, l_ref)
    out_ref[...] = jnp.broadcast_to(l_ref[...][None], out_ref.shape)


def later_columns(parts_ref, half_ref, b_ref, norm_ref, every_ref, out_ref, a_ref, d_ref, l_ref):
    every = merged(parts_ref[...]) - norm_ref[0:1, :]
    every_ref[...] = every
    fill_left(a_ref, half_ref[...])
    place_terms(a_ref, d_ref, -math.log2(NSRC * lax.axis_size("src")) - every, SRC_TILES)
    log_sums(half_ref, a_ref, b_ref, l_ref)
    out_ref[...] = jnp.broadcast_to(l_ref[...][None], out_ref.shape)


def last_columns(parts_ref, far_ref, every_ref, near_ref, f_ref, g_ref):
    f_ref[...] = near_ref[...] - UNKAPPA * every_ref[...]
    g_ref[...] = far_ref[...] - UNKAPPA * merged(parts_ref[...])


def shape(dims, kind=f32):
    return jax.ShapeDtypeStruct(dims, kind)


def call(body, outs, inputs, scratch=(), space=pltpu.VMEM):
    if space is pltpu.HBM:
        inputs = [pltpu.with_memory_space_constraint(x, space) for x in inputs]
    return pl.pallas_call(
        body,
        out_shape=outs,
        in_specs=[pl.BlockSpec(memory_space=space)] * len(inputs),
        out_specs=jax.tree.map(lambda _: pl.BlockSpec(memory_space=pltpu.VMEM), outs),
        scratch_shapes=scratch,
        name=body.__name__,
        compiler_params=pltpu.CompilerParams(vmem_limit_bytes=GRANT),
    )(*inputs)


def exchanged(x, axis):
    return lax.all_to_all(
        x, axis, split_axis=0, concat_axis=0, axis_index_groups=[ORDER[axis]], tiled=True
    )


def local(generator, shift, targets, log_weights):
    n_src, n_tgt = lax.axis_size("src"), lax.axis_size("tgt")
    f_tmp = lambda rows: [
        pltpu.VMEM((NTGT, LANES), bf16),
        pltpu.VMEM((TGT_TILES, 8, LANES), f32),
        pltpu.VMEM((rows, LANES), f32),
    ]
    g_tmp = [
        pltpu.VMEM((NSRC, LANES), bf16),
        pltpu.VMEM((SRC_TILES, 8, LANES), f32),
        pltpu.VMEM((TGT_TILES, LANES), f32),
    ]
    w = log_weights.reshape(TGT_TILES, LANES)
    f_half, f_right, g_half, g_right, c, far, near, part = call(
        first_rows,
        (
            shape((NTGT, LANES), bf16),
            shape((256, NSRC), bf16),
            shape((NSRC, LANES), bf16),
            shape((256, NTGT), bf16),
            shape((TGT_TILES, LANES)),
            shape((TGT_TILES, LANES)),
            shape((SRC_TILES, LANES)),
            shape((n_tgt * FIRST_ROWS, LANES)),
        ),
        (generator, shift, targets, w),
        f_tmp(SRC_TILES + 8)
        + [
            pltpu.SMEM((DIM,), jnp.int32),
            pltpu.SMEM((DIM,), f32),
            pltpu.VMEM((DIM, NTGT), f32),
            pltpu.VMEM((TGT_TILES, LANES), f32),
            pltpu.SemaphoreType.DMA((3 + SPLIT,)),
        ],
        space=pltpu.HBM,
    )
    part = part.reshape(n_tgt, 1, FIRST_ROWS * LANES)
    got = exchanged(part, "tgt").reshape(n_tgt * FIRST_ROWS, LANES)
    norm, part = call(
        first_columns,
        (shape((8, LANES)), shape((n_src, TGT_TILES, LANES))),
        (got, g_half, g_right),
        g_tmp,
    )
    got = exchanged(part, "src")
    part = call(
        later_rows, shape((n_tgt, SRC_TILES, LANES)), (got, f_half, f_right, c), f_tmp(SRC_TILES)
    )
    got = exchanged(part, "tgt")
    every, part = call(
        later_columns,
        (shape((SRC_TILES, LANES)), shape((n_src, TGT_TILES, LANES))),
        (got, g_half, g_right, norm),
        g_tmp,
    )
    got = exchanged(part, "src")
    f, g = call(
        last_columns,
        (shape((SRC_TILES, LANES)), shape((TGT_TILES, LANES))),
        (got, far, every, near),
    )
    return f.reshape(NSRC), g.reshape(NTGT)


def solution(mesh):
    in_specs = (P(), P(), P(None, "tgt"), P("tgt"))
    out_specs = (P("src"), P("tgt"))
    return jax.shard_map(local, mesh=mesh, in_specs=in_specs, out_specs=out_specs, check_vma=False)
```

```python
import math
import jax
import jax.numpy as jnp
from jax import lax
from jax.experimental import pallas as pl
from jax.experimental.pallas import tpu as pltpu
from jax.sharding import PartitionSpec as P

DIM = 64
NSRC = 2048
NTGT = 1024
LANES = 128
SRC_TILES = NSRC // LANES
TGT_TILES = NTGT // LANES
FIRST_ROWS = SRC_TILES + 1
BLUR = 0.1
LOG2E = 1.4426950408889634
KAPPA = LOG2E / BLUR
UNKAPPA = 1.0 / KAPPA
WIDTH = 256
ROWS = 64
EARLY = 4
GRANT = 16 * 2**20
ORDER = {"src": [4, 0, 1, 7, 2, 6, 3, 5], "tgt": [(21 + k) % 32 for k in range(32)]}
f32 = jnp.float32
bf16 = jnp.bfloat16

SINE = (6.28318530707259, -41.34170211699658, 81.6052262062997, -76.7042813207251, 42.00980570831026, -14.394135222236105)


def split(x):
    hi = x.astype(bf16)
    lo = (x - hi.astype(f32)).astype(bf16)
    return hi, lo


def pieces(x):
    first = x.astype(bf16).astype(f32)
    rest = x - first
    second = rest.astype(bf16).astype(f32)
    return first, second, rest - second


def column_of(values, kind):
    sub = lax.broadcasted_iota(jnp.int32, (8, LANES), 0)
    groups = []
    for g in range(DIM // 8):
        v = jnp.full((8, LANES), values[8 * g], kind)
        for s in range(1, 8):
            v = jnp.where(sub == s, values[8 * g + s], v)
        groups.append(v)
    return jnp.concatenate(groups, 0)


def sine_turns(u):
    r = u - jnp.floor(u + 0.5)
    a = jnp.abs(r)
    b = jnp.minimum(a, 0.5 - a)
    z = b * b
    p = jnp.full_like(z, SINE[-1])
    for c in SINE[-2::-1]:
        p = p * z + c
    v = b * p
    return jnp.where(r < 0, -v, v)


def place_terms(a_ref, d_ref, rows, tiles):
    d_ref[...] = jnp.zeros_like(d_ref)
    for k, piece in enumerate(pieces(rows)):
        d_ref[:, k, :] = piece
    for t in range(tiles):
        a_ref[LANES * t : LANES * (t + 1), 0:8] = d_ref[t].T.astype(bf16)


def fill_left(a_ref, half):
    lane = lax.broadcasted_iota(jnp.int32, half.shape, 1)
    a_ref[...] = jnp.where(lane < 64, jnp.zeros_like(half), half)


def log_sums(half_ref, a_ref, b_ref, out):
    for n in range(b_ref.shape[1] // WIDTH):
        a = jnp.concatenate([half_ref[...], a_ref[...]], 1)
        s = jnp.dot(a, b_ref[:, WIDTH * n : WIDTH * (n + 1)], preferred_element_type=f32)
        found = [([], []) for _ in range(WIDTH // LANES)]
        for m in range(0, s.shape[0], ROWS):
            for k, (tops, sums) in enumerate(found):
                block = s[m : m + ROWS, LANES * k : LANES * (k + 1)].reshape(ROWS // 8, 8, LANES)
                top = jnp.max(block, 0)
                tops.append(top)
                sums.append(jnp.sum(jnp.exp2(block - top[None]), 0))
        for k, (tops, sums) in enumerate(found):
            tops, sums = jnp.concatenate(tops, 0), jnp.concatenate(sums, 0)
            top = jnp.max(tops, 0, keepdims=True)
            r = n * (WIDTH // LANES) + k
            out[r : r + 1, :] = top + jnp.log2(jnp.sum(sums * jnp.exp2(tops - top), 0, keepdims=True))


def merged(parts):
    top = jnp.max(parts, 0)
    return top + jnp.log2(jnp.sum(jnp.exp2(parts - top[None]), 0))


def ones_rows():
    row = lax.broadcasted_iota(jnp.int32, (64, LANES), 0)
    return jnp.where(row < 3, 1.0, 0.0).astype(bf16)


def first_rows(
    gen_hbm, shift_hbm, t_hbm, w_hbm,
    half_ref, b_ref, g_half_ref, g_b_ref, c_ref, far_ref, near_ref, out_ref,
    a_ref, d_ref, l_ref, gen, shift, t_ref, w_ref, sems,
):
    moves = [
        pltpu.make_async_copy(src, dst, sems.at[k])
        for k, (src, dst) in enumerate(
            ((gen_hbm, gen), (shift_hbm, shift), (t_hbm, t_ref), (w_hbm, w_ref))
        )
    ]
    for k in (2, 0, 1, 3):
        moves[k].start()
    ones = ones_rows()
    for t in range(SRC_TILES):
        b_ref[128:192, LANES * t : LANES * (t + 1)] = ones
    for t in range(TGT_TILES):
        g_b_ref[128:192, LANES * t : LANES * (t + 1)] = ones
    offset = lax.axis_index("src") * NSRC
    modulus = NSRC * lax.axis_size("src")
    moves[0].wait()
    moves[1].wait()
    g = column_of(gen, jnp.int32)
    sh = column_of(shift, f32)
    lane = lax.broadcasted_iota(jnp.int32, (DIM, LANES), 1)
    turns = (((offset + lane) * g) & (modulus - 1)).astype(f32) * (1.0 / modulus) + sh
    step = ((LANES * g) & (modulus - 1)).astype(f32) * (1.0 / modulus)
    scaled, other = KAPPA * sine_turns(turns), KAPPA * sine_turns(turns + 0.25)
    step_sin, step_cos = sine_turns(step), sine_turns(step + 0.25)
    def put(t, scaled, other):
        cols = slice(LANES * t, LANES * (t + 1))
        near_ref[t : t + 1, :] = (0.5 * UNKAPPA**2) * jnp.sum(scaled * scaled, 0, keepdims=True)
        hi = scaled.astype(bf16).astype(f32)
        lo = scaled - hi
        b_ref[0:64, cols] = hi.astype(bf16)
        b_ref[64:128, cols] = hi.astype(bf16)
        b_ref[192:256, cols] = lo.astype(bf16)
        g_half_ref[cols, :] = jnp.concatenate([lo, hi], 0).T.astype(bf16)
        return scaled * step_cos + other * step_sin, other * step_cos - scaled * step_sin

    for t in range(EARLY):
        scaled, other = put(t, scaled, other)
    moves[2].wait()
    moves[3].wait()
    w = w_ref[...] * LOG2E
    c_ref[...] = w
    for t in range(TGT_TILES):
        rows = slice(LANES * t, LANES * (t + 1))
        y = t_ref[:, rows]
        far_ref[t : t + 1, :] = 0.5 * jnp.sum(y * y, 0, keepdims=True)
        hi = y.astype(bf16).astype(f32)
        half_ref[rows, :] = jnp.concatenate([y - hi, hi], 0).T.astype(bf16)
        g_b_ref[0:64, rows] = hi.astype(bf16)
        g_b_ref[64:128, rows] = hi.astype(bf16)
        g_b_ref[192:256, rows] = (y - hi).astype(bf16)
    fill_left(a_ref, half_ref[...])
    place_terms(a_ref, d_ref, w - KAPPA * far_ref[...], TGT_TILES)
    for t in range(EARLY, SRC_TILES):
        scaled, other = put(t, scaled, other)
    top = jnp.max(w, keepdims=True)
    total = top + jnp.log2(jnp.sum(jnp.exp2(w - top), keepdims=True))
    log_sums(half_ref, a_ref, b_ref, l_ref)
    l_ref[SRC_TILES:, :] = jnp.broadcast_to(total, (8, LANES))
    for d in range(0, out_ref.shape[0], FIRST_ROWS):
        out_ref[d : d + FIRST_ROWS, :] = l_ref[:FIRST_ROWS, :]


def first_columns(parts_ref, half_ref, b_ref, norm_ref, out_ref, a_ref, d_ref, l_ref):
    parts = [parts_ref[d : d + FIRST_ROWS, :] for d in range(0, parts_ref.shape[0], FIRST_ROWS)]
    top = parts[0]
    for part in parts[1:]:
        top = jnp.maximum(top, part)
    every = top + jnp.log2(sum(jnp.exp2(part - top) for part in parts))
    norm = every[SRC_TILES:, :]
    norm_ref[...] = jnp.broadcast_to(norm, norm_ref.shape)
    rows = (norm - every[:SRC_TILES, :]) - math.log2(NSRC * lax.axis_size("src"))
    fill_left(a_ref, half_ref[...])
    place_terms(a_ref, d_ref, rows, SRC_TILES)
    log_sums(half_ref, a_ref, b_ref, l_ref)
    out_ref[...] = jnp.broadcast_to(l_ref[...][None], out_ref.shape)


def later_rows(parts_ref, half_ref, b_ref, c_ref, out_ref, a_ref, d_ref, l_ref):
    rows = c_ref[...] - merged(parts_ref[...])
    fill_left(a_ref, half_ref[...])
    place_terms(a_ref, d_ref, rows, TGT_TILES)
    log_sums(half_ref, a_ref, b_ref, l_ref)
    out_ref[...] = jnp.broadcast_to(l_ref[...][None], out_ref.shape)


def later_columns(parts_ref, half_ref, b_ref, norm_ref, every_ref, out_ref, a_ref, d_ref, l_ref):
    every = merged(parts_ref[...]) - norm_ref[0:1, :]
    every_ref[...] = every
    fill_left(a_ref, half_ref[...])
    place_terms(a_ref, d_ref, -math.log2(NSRC * lax.axis_size("src")) - every, SRC_TILES)
    log_sums(half_ref, a_ref, b_ref, l_ref)
    out_ref[...] = jnp.broadcast_to(l_ref[...][None], out_ref.shape)


def last_columns(parts_ref, far_ref, every_ref, near_ref, f_ref, g_ref):
    f_ref[...] = near_ref[...] - UNKAPPA * every_ref[...]
    g_ref[...] = far_ref[...] - UNKAPPA * merged(parts_ref[...])


def shape(dims, kind=f32):
    return jax.ShapeDtypeStruct(dims, kind)


def call(body, outs, inputs, scratch=(), space=pltpu.VMEM):
    if space is pltpu.HBM:
        inputs = [pltpu.with_memory_space_constraint(x, space) for x in inputs]
    return pl.pallas_call(
        body,
        out_shape=outs,
        in_specs=[pl.BlockSpec(memory_space=space)] * len(inputs),
        out_specs=jax.tree.map(lambda _: pl.BlockSpec(memory_space=pltpu.VMEM), outs),
        scratch_shapes=scratch,
        name=body.__name__,
        compiler_params=pltpu.CompilerParams(vmem_limit_bytes=GRANT),
    )(*inputs)


def exchanged(x, axis):
    return lax.all_to_all(
        x, axis, split_axis=0, concat_axis=0, axis_index_groups=[ORDER[axis]], tiled=True
    )


def local(generator, shift, targets, log_weights):
    n_src, n_tgt = lax.axis_size("src"), lax.axis_size("tgt")
    f_tmp = lambda rows: [
        pltpu.VMEM((NTGT, LANES), bf16),
        pltpu.VMEM((TGT_TILES, 8, LANES), f32),
        pltpu.VMEM((rows, LANES), f32),
    ]
    g_tmp = [
        pltpu.VMEM((NSRC, LANES), bf16),
        pltpu.VMEM((SRC_TILES, 8, LANES), f32),
        pltpu.VMEM((TGT_TILES, LANES), f32),
    ]
    w = log_weights.reshape(TGT_TILES, LANES)
    f_half, f_right, g_half, g_right, c, far, near, part = call(
        first_rows,
        (
            shape((NTGT, LANES), bf16),
            shape((256, NSRC), bf16),
            shape((NSRC, LANES), bf16),
            shape((256, NTGT), bf16),
            shape((TGT_TILES, LANES)),
            shape((TGT_TILES, LANES)),
            shape((SRC_TILES, LANES)),
            shape((n_tgt * FIRST_ROWS, LANES)),
        ),
        (generator, shift, targets, w),
        f_tmp(SRC_TILES + 8)
        + [
            pltpu.SMEM((DIM,), jnp.int32),
            pltpu.SMEM((DIM,), f32),
            pltpu.VMEM((DIM, NTGT), f32),
            pltpu.VMEM((TGT_TILES, LANES), f32),
            pltpu.SemaphoreType.DMA((4,)),
        ],
        space=pltpu.HBM,
    )
    part = part.reshape(n_tgt, 1, FIRST_ROWS * LANES)
    got = exchanged(part, "tgt").reshape(n_tgt * FIRST_ROWS, LANES)
    norm, part = call(
        first_columns,
        (shape((8, LANES)), shape((n_src, TGT_TILES, LANES))),
        (got, g_half, g_right),
        g_tmp,
    )
    got = exchanged(part, "src")
    part = call(
        later_rows, shape((n_tgt, SRC_TILES, LANES)), (got, f_half, f_right, c), f_tmp(SRC_TILES)
    )
    got = exchanged(part, "tgt")
    every, part = call(
        later_columns,
        (shape((SRC_TILES, LANES)), shape((n_src, TGT_TILES, LANES))),
        (got, g_half, g_right, norm),
        g_tmp,
    )
    got = exchanged(part, "src")
    f, g = call(
        last_columns,
        (shape((SRC_TILES, LANES)), shape((TGT_TILES, LANES))),
        (got, far, every, near),
    )
    return f.reshape(NSRC), g.reshape(NTGT)


def solution(mesh):
    in_specs = (P(), P(), P(None, "tgt"), P("tgt"))
    out_specs = (P("src"), P("tgt"))
    return jax.shard_map(local, mesh=mesh, in_specs=in_specs, out_specs=out_specs, check_vma=False)
```
